32 devices in a mesh: gz: 8 (over z, y), gy: 4 (over x, core).
Axes of the slice: x: 2, y: 2, z: 4, core: 2. Of those that a mesh axis runs over, the one named last changes fastest.
Arguments:
- charge: float32 [393216], P(('gz', 'gy')), may hold values from -4 to 4
- fractions: float32 [3, 393216], P(None, ('gz', 'gy')), may hold values from 0 to 1
- cell_base: int32 [3, 393216], P(None, ('gz', 'gy')), may hold values from 0 to 255, as said below
- live_blocks: int32 [8, 4], P('gz'), may hold values from 12 to 96, as said below
- send_blocks: int32 [8, 4], P('gz'), may hold values from 0 to 36, as said below
- moduli: float32 [3, 256], replicated, may hold values from 0.5 to 2
- screening: float32 [1], replicated, may hold values from 8 to 16
Outputs:
- forces: float32 [3, 393216], P(None, ('gz', 'gy'))
The draws below stay inside these ranges and needn't reach their ends.
Inputs may be any that keep to these rules, and one draw needn't show every extreme that they name: `cell_base`: row 0 lies in 0 to 31, row 1 in 0 to 63, row 2 in 0 to 255. `live_blocks`: a domain's live blocks are its first ones; in every row of the table some domain has 96 live blocks. send_blocks is at most the domain's live blocks; live_blocks minus send_blocks plus send_blocks of the domain before it along gy (cyclically) is at most 96; in every row some domain sends 36.
All inputs are finite; a program needn't handle non-finite values.
Results may differ from the reference program's by a relative error of at most 0.00023.
Values sent between devices are 32-bit elements; how exact they have to be, the bound alone decides.
A program may use at most 128 MiB of HBM per device.

```python
import math
import jax
import jax.numpy as jnp

GRID = 256
BLOCK = 128
NBLK = 96
ATOMS_DEV = 12288
ATOMS = 393216
PZ = 32
PY = 64
SEND_MAX = 36
LOW = 12
N_GZ = 8
N_GY = 4


def migration_plan(key):
    base_key = jax.random.fold_in(key, 7)
    key_load, key_busy = jax.random.split(base_key)
    drawn = jax.random.randint(key_load, (N_GZ, N_GY), 0, 1001)
    powered = drawn * drawn // 1000
    powered = powered * powered // 1000
    live_count = LOW + (NBLK - LOW) * powered // 1000
    busiest = jax.random.randint(key_busy, (N_GZ, 1), 0, N_GY)
    lane_ids = jnp.arange(N_GY, dtype=jnp.int32)[None, :]
    live_count = jnp.where(lane_ids == busiest, NBLK, live_count)
    live_count = jnp.where(lane_ids == jnp.mod(busiest + 1, N_GY), LOW, live_count)
    following = jnp.roll(live_count, -1, axis=1)
    send_count = jnp.clip((live_count - following + 1) // 2, 0, SEND_MAX)
    return (live_count.astype(jnp.int32), send_count.astype(jnp.int32))


def draw_live_blocks(key, part):
    return migration_plan(key)[0]


def draw_send_blocks(key, part):
    return migration_plan(key)[1]


def draw_cell_base(key, part):
    key_z, key_y, key_x = jax.random.split(jax.random.fold_in(key, 11), 3)
    rows_z = jax.random.randint(key_z, (ATOMS,), 0, PZ)
    rows_y = jax.random.randint(key_y, (ATOMS,), 0, PY)
    rows_x = jax.random.randint(key_x, (ATOMS,), 0, GRID)
    return jnp.stack([rows_z, rows_y, rows_x]).astype(jnp.int32)


def steps_of(key, extent, cuts, low, high):
    def one(axis_at, shards_of):
        draws = jax.random.uniform(jax.random.fold_in(jax.random.fold_in(key, 6), axis_at), (shards_of,), jnp.float32, low / len(cuts), high / len(cuts))
        return jnp.repeat(jnp.exp(draws), extent[axis_at] // shards_of).reshape((-1,) + (1,) * (len(extent) - axis_at - 1))

    level = one(*cuts[0])
    for cut in cuts[1:]:
        level = level * one(*cut)
    return level


def normal_values(stream_key, shape, scale, limit, shards=(), held_as=jnp.bfloat16):
    factor_of = steps_of(stream_key, shape, shards, -0.22, 0.18) if shards else 1.0
    array = jax.random.normal(stream_key, shape, jnp.float32) * scale * factor_of
    return jnp.minimum(jnp.maximum(array, -limit), limit).astype(held_as)


def setup_inputs(seed: int = 0) -> dict:
    splits = jax.random.split(jax.random.key(seed), 8)
    charge = normal_values(splits[0], (ATOMS,), 1.0, 4.0, ((0, 32),), jnp.float32)
    fractions = jnp.clip(1.0 * jax.random.uniform(splits[1], (3, ATOMS), jnp.float32) ** steps_of(splits[1], (3, ATOMS), ((1, 32),), -0.2, 0.2), 0.0, 1.0)
    cell_base = draw_cell_base(jax.random.fold_in(splits[7], 71), 0)
    live_blocks = draw_live_blocks(jax.random.fold_in(splits[7], 71), 0)
    send_blocks = draw_send_blocks(jax.random.fold_in(splits[7], 71), 0)
    moduli = jnp.clip(jnp.exp(jax.random.uniform(splits[5], (3, GRID), jnp.float32, math.log(0.5), math.log(2.0))), 0.5, 2.0)
    screening = jnp.clip(jnp.exp(jax.random.uniform(splits[6], (1,), jnp.float32, math.log(8.0), math.log(16.0))), 8.0, 16.0)
    return {"charge": charge, "fractions": fractions, "cell_base": cell_base, "live_blocks": live_blocks, "send_blocks": send_blocks, "moduli": moduli, "screening": screening}


coulomb = 2.0


def spline_weights(fractions_row):
    remain = 1.0 - fractions_row
    square = fractions_row * fractions_row
    cubed = square * fractions_row
    weights = [remain * remain * remain / 6.0,
               (3.0 * cubed - 6.0 * square + 4.0) / 6.0,
               (-3.0 * cubed + 3.0 * square + 3.0 * fractions_row + 1.0) / 6.0,
               cubed / 6.0]
    slopes = [-0.5 * remain * remain,
              1.5 * square - 2.0 * fractions_row,
              -1.5 * square + fractions_row + 0.5,
              0.5 * square]
    return weights, slopes


def reference(charge, fractions, cell_base, live_blocks, send_blocks, moduli, screening):
    atom_index = jnp.arange(ATOMS, dtype=jnp.int32)
    device_index = atom_index // ATOMS_DEV
    slab_index = device_index // N_GY
    column_index = device_index % N_GY
    slot_index = atom_index % ATOMS_DEV
    live_count = live_blocks[slab_index, column_index]
    weighted = jnp.where(slot_index // BLOCK < live_count, charge, 0.0)
    weight_z, slope_z = spline_weights(fractions[0])
    weight_y, slope_y = spline_weights(fractions[1])
    weight_x, slope_x = spline_weights(fractions[2])
    base_z = slab_index * PZ + cell_base[0]
    base_y = column_index * PY + cell_base[1]
    base_x = cell_base[2]
    density = jnp.zeros((GRID * GRID * GRID,), jnp.float32)
    for shift_z in range(4):
        index_z = jnp.mod(base_z + shift_z, GRID)
        for shift_y in range(4):
            index_y = jnp.mod(base_y + shift_y, GRID)
            for shift_x in range(4):
                index_x = jnp.mod(base_x + shift_x, GRID)
                flat_index = ((index_z * GRID + index_y) * GRID + index_x).astype(jnp.int32)
                density = density.at[flat_index].add(weighted * weight_z[shift_z] * weight_y[shift_y] * weight_x[shift_x])
    density = density.reshape(GRID, GRID, GRID)
    spectrum = jnp.fft.fftn(density)
    waves = jnp.arange(GRID, dtype=jnp.int32)
    signed_wave = jnp.where(waves < GRID // 2, waves, waves - GRID)
    wave_square = signed_wave * signed_wave
    radius = wave_square[:, None, None] + wave_square[None, :, None] + wave_square[None, None, :]
    squared = radius.astype(jnp.float32) / float(GRID * GRID)
    product = coulomb * moduli[0][:, None, None] * moduli[1][None, :, None] * moduli[2][None, None, :]
    safe_squared = jnp.where(radius > 0, squared, 1.0)
    kernel = jnp.where(radius > 0, product * jnp.exp(-screening[0] * squared) / safe_squared, 0.0)
    potential = jnp.real(jnp.fft.ifftn(spectrum * kernel)).astype(jnp.float32)
    flat_potential = potential.reshape(-1)
    force_z = jnp.zeros((ATOMS,), jnp.float32)
    force_y = jnp.zeros((ATOMS,), jnp.float32)
    force_x = jnp.zeros((ATOMS,), jnp.float32)
    for shift_z in range(4):
        index_z = jnp.mod(base_z + shift_z, GRID)
        for shift_y in range(4):
            index_y = jnp.mod(base_y + shift_y, GRID)
            for shift_x in range(4):
                index_x = jnp.mod(base_x + shift_x, GRID)
                flat_index = ((index_z * GRID + index_y) * GRID + index_x).astype(jnp.int32)
                values = flat_potential[flat_index]
                force_z = force_z + slope_z[shift_z] * weight_y[shift_y] * weight_x[shift_x] * values
                force_y = force_y + weight_z[shift_z] * slope_y[shift_y] * weight_x[shift_x] * values
                force_x = force_x + weight_z[shift_z] * weight_y[shift_y] * slope_x[shift_x] * values
    home = -weighted[None, :] * jnp.stack([force_z, force_y, force_x])
    domains = N_GZ * N_GY
    home = home.reshape(3, domains, ATOMS_DEV)
    live_flat = live_blocks.reshape(-1)
    send_flat = send_blocks.reshape(-1)
    devices = jnp.arange(domains, dtype=jnp.int32)
    column_of = devices % N_GY
    previous = (devices - column_of + jnp.mod(column_of - 1, N_GY)).astype(jnp.int32)
    kept_atoms = (live_flat - send_flat) * BLOCK
    arriving = send_flat[previous] * BLOCK
    source_start = (live_flat[previous] - send_flat[previous]) * BLOCK
    slots = jnp.arange(ATOMS_DEV, dtype=jnp.int32)
    own_forces = jnp.where(slots[None, None, :] < kept_atoms[None, :, None], home, 0.0)
    guest_slot = slots[None, :] - kept_atoms[:, None] + source_start[:, None]
    valid = (slots[None, :] >= kept_atoms[:, None]) & (slots[None, :] < kept_atoms[:, None] + arriving[:, None])
    guest_slot = jnp.clip(guest_slot, 0, ATOMS_DEV - 1).astype(jnp.int32)
    neighbour = home[:, previous, :]
    guest = jnp.take_along_axis(neighbour, guest_slot[None, :, :], axis=2)
    result = own_forces + jnp.where(valid[None, :, :], guest, 0.0)
    return result.reshape(3, ATOMS)
```

```python
import functools

import jax
import jax.numpy as jnp
import numpy as np
from jax import lax
from jax.experimental import pallas as pl
from jax.experimental.pallas import tpu as pltpu
from jax.sharding import PartitionSpec as P

BLOCK = 128
SEND_MAX = 36
GROUP = 256
PAIR = 2
LAYER = 2
STEP = 7
WINDOW = 24
CHUNKS = 4
DEAD = 1 << 30

high = lax.Precision.HIGH
coulomb = 2.0


def shifted(x, axis, by):
    peers = lax.axis_size(axis)
    return lax.ppermute(x, axis, [(i, (i + by) % peers) for i in range(peers)])


def round_up(value, step):
    return -(-value // step) * step


def spline_weights(t):
    remain = 1.0 - t
    square = t * t
    cubed = square * t
    weights = [
        remain * remain * remain * (1.0 / 6.0),
        (3.0 * cubed - 6.0 * square + 4.0) * (1.0 / 6.0),
        (-3.0 * cubed + 3.0 * square + 3.0 * t + 1.0) * (1.0 / 6.0),
        cubed * (1.0 / 6.0),
    ]
    slopes = [
        -0.5 * remain * remain,
        1.5 * square - 2.0 * t,
        -1.5 * square + t + 0.5,
        0.5 * square,
    ]
    return weights, slopes


def stencil(base, weights, span):
    offset = lax.broadcasted_iota(jnp.int32, (span, base.shape[1]), 0) - base
    table = jnp.where(offset == 0, weights[0], 0.0)
    for k in range(1, 4):
        table = jnp.where(offset == k, weights[k], table)
    return table


def split(value):
    top = value.astype(jnp.bfloat16)
    rest = (value - top.astype(jnp.float32)).astype(jnp.bfloat16)
    return top, rest


def encode(cells, bits_y, bits_x):
    layer = cells[0] >> LAYER
    flip = (layer & 1) * ((1 << bits_y) - 1)
    inner = cells[0] & ((1 << LAYER) - 1)
    key = (layer << bits_y) | (cells[1] ^ flip)
    return (((key << LAYER) | inner) << bits_x) | cells[2]


def decode(key, bits_y, bits_x):
    inner = (key >> bits_x) & ((1 << LAYER) - 1)
    y = (key >> (bits_x + LAYER)) & ((1 << bits_y) - 1)
    layer = key >> (bits_x + LAYER + bits_y)
    y = y ^ ((layer & 1) * ((1 << bits_y) - 1))
    return (layer << LAYER) | inner, y, key & ((1 << bits_x) - 1)


def wrapped_stencil(places, base, weights, grid):
    top_table = rest_table = jnp.zeros(places.shape, jnp.bfloat16)
    for k in range(4):
        at = base + k
        at = jnp.where(at >= grid, at - grid, at).astype(jnp.float32).astype(jnp.bfloat16)
        hit = places == at
        top, rest = split(weights[k])
        top_table = jnp.where(hit, top, top_table)
        rest_table = jnp.where(hit, rest, rest_table)
    return top_table, rest_table


def fill_places(places):
    places[...] = (
        lax.broadcasted_iota(jnp.int32, places.shape, 0).astype(jnp.float32).astype(jnp.bfloat16)
    )


def over_windows(bounds, group, visit):
    low_z, high_z, low_y, high_y = (bounds[i, group] for i in range(4))
    start = (low_y // 8) * 8
    steps = (high_z + 3 - low_z) // STEP + 1
    strips = (high_y + 3 - start) // WINDOW + 1
    visit(low_z, start)

    def rest():
        @pl.loop(1, steps * strips)
        def _(at):
            visit(low_z + lax.rem(at, steps) * STEP, start + lax.div(at, steps) * WINDOW)

    return rest


def over_groups(atoms, prepare):
    @pl.loop(0, (atoms + PAIR * GROUP - 1) // (PAIR * GROUP))
    def _(turn):
        later = [prepare(turn * PAIR + i, i) for i in range(PAIR)]
        for rest in later:
            rest()


def spread_kernel(
    rows, grid, bits, count, bounds, key, charge, fz, fy, fx, tile, places, table_z, factor_x,
):
    tile[...] = jnp.zeros_like(tile)
    fill_places(places)
    atoms = count[0]

    def prepare(group, lane):
        at = pl.ds(pl.multiple_of(group * GROUP, GROUP), GROUP)
        place = group * GROUP + lax.broadcasted_iota(jnp.int32, (1, GROUP), 1)
        value = jnp.where(place < atoms, charge[0:1, at], 0.0)
        cell_z, cell_y, cell_x = decode(key[0:1, at], *bits)
        weight_z, _ = spline_weights(fz[0:1, at])
        weight_y, _ = spline_weights(fy[0:1, at])
        weight_x, _ = spline_weights(fx[0:1, at])
        weight_x = [value * w for w in weight_x]
        top, rest = wrapped_stencil(places[...], cell_x, weight_x, grid)
        factor_x[lane, :, :GROUP] = top
        factor_x[lane, :, GROUP:] = rest

        def visit(first, start):
            table_z[lane] = stencil(cell_z - first, weight_z, table_z.shape[1])
            table_y = stencil(cell_y - start, weight_y, WINDOW)
            part = jnp.concatenate([table_z[lane, j : j + 1, :] * table_y for j in range(STEP)], 0)
            top, rest = split(part)
            across = (((1,), (1,)), ((), ()))
            values = lax.dot_general(
                jnp.concatenate([top, rest], 0), factor_x[lane, :, :GROUP], across,
                preferred_element_type=jnp.float32,
            )
            values = values[: STEP * WINDOW] + values[STEP * WINDOW :] + lax.dot_general(
                top, factor_x[lane, :, GROUP:], across, preferred_element_type=jnp.float32
            )
            for j in range(STEP):
                where = pl.ds(pl.multiple_of((first + j) * rows + start, 8), WINDOW)
                tile[where, :] += values[j * WINDOW : (j + 1) * WINDOW, :]

        return over_windows(bounds, group, visit)

    over_groups(atoms, prepare)


def interpolate_kernel(
    rows, grid, bits, count, bounds, key, charge, fz, fy, fx, tile, force_z, force_y, force_x,
    places, factor_x, table_z, rising_z, total,
):
    force_z[...] = jnp.zeros_like(force_z)
    force_y[...] = jnp.zeros_like(force_y)
    force_x[...] = jnp.zeros_like(force_x)
    fill_places(places)
    atoms = count[0]

    def prepare(group, lane):
        at = pl.ds(pl.multiple_of(group * GROUP, GROUP), GROUP)
        place = group * GROUP + lax.broadcasted_iota(jnp.int32, (1, GROUP), 1)
        value = -jnp.where(place < atoms, charge[0:1, at], 0.0)
        cell_z, cell_y, cell_x = decode(key[0:1, at], *bits)
        weight_z, slope_z = spline_weights(fz[0:1, at])
        weight_y, slope_y = spline_weights(fy[0:1, at])
        weight_x, slope_x = spline_weights(fx[0:1, at])
        for half, values in enumerate((weight_x, slope_x)):
            top, rest = wrapped_stencil(places[...], cell_x, values, grid)
            columns = slice(half * GROUP, (half + 1) * GROUP)
            factor_x[lane, :grid, columns] = top
            factor_x[lane, grid:, columns] = rest
        total[lane] = jnp.zeros(total.shape[1:], jnp.float32)

        def visit(first, start):
            span = table_z.shape[1]
            table_z[lane] = stencil(cell_z - first, weight_z, span)
            rising_z[lane] = stencil(cell_z - first, slope_z, span)
            top, rest = split(
                jnp.concatenate(
                    [
                        tile[pl.ds(pl.multiple_of((first + j) * rows + start, 8), WINDOW), :]
                        for j in range(STEP)
                    ],
                    0,
                )
            )
            along = jnp.dot(
                jnp.concatenate([top, rest], 0), factor_x[lane, :grid, :],
                preferred_element_type=jnp.float32,
            )
            along = along[: STEP * WINDOW] + along[STEP * WINDOW :] + jnp.dot(
                top, factor_x[lane, grid:, :], preferred_element_type=jnp.float32
            )
            table_y = stencil(cell_y - start, weight_y, WINDOW)
            rising_y = stencil(cell_y - start, slope_y, WINDOW)
            zs = [table_z[lane, j : j + 1, :] for j in range(STEP)]
            gs = [rising_z[lane, j : j + 1, :] for j in range(STEP)]
            sums = [0.0, 0.0, 0.0]
            for r in range(0, WINDOW, 8):
                local = slice(r, r + 8)
                w = [along[j * WINDOW + r : j * WINDOW + r + 8, :GROUP] for j in range(STEP)]
                s = [along[j * WINDOW + r : j * WINDOW + r + 8, GROUP:] for j in range(STEP)]
                sums[0] += table_y[local] * sum(gs[j] * w[j] for j in range(STEP))
                sums[1] += rising_y[local] * sum(zs[j] * w[j] for j in range(STEP))
                sums[2] += table_y[local] * sum(zs[j] * s[j] for j in range(STEP))
            for i in range(3):
                total[lane, 8 * i : 8 * i + 8, :] += sums[i]

        rest_of = over_windows(bounds, group, visit)

        def finish():
            rest_of()
            for i, force in enumerate((force_z, force_y, force_x)):
                part = total[lane, 8 * i : 8 * i + 8, :]
                force[0:1, at] = value * jnp.sum(part, 0, keepdims=True)

        return finish

    over_groups(atoms, prepare)


def vmem():
    return pl.BlockSpec(memory_space=pltpu.VMEM)


def smem():
    return pl.BlockSpec(memory_space=pltpu.SMEM)


def spread_atoms(count, bounds, atoms, bits, planes, rows, grid):
    slots = atoms[0].shape[1]
    return pl.pallas_call(
        functools.partial(spread_kernel, rows, grid, bits),
        out_shape=jax.ShapeDtypeStruct((planes * rows, grid), jnp.float32),
        in_specs=[smem()] * 2 + [vmem()] * 5,
        out_specs=vmem(),
        scratch_shapes=[
            pltpu.VMEM((grid, GROUP), jnp.bfloat16),
            pltpu.VMEM((PAIR, 8, GROUP), jnp.float32),
            pltpu.VMEM((PAIR, grid, 2 * GROUP), jnp.bfloat16),
        ],
        cost_estimate=pl.CostEstimate(
            flops=STEP * rows * grid * slots * 6,
            bytes_accessed=planes * rows * grid * 4,
            transcendentals=0,
        ),
        name="spread",
    )(count, bounds, *atoms)


def interpolate_atoms(count, bounds, atoms, tile, bits, planes, rows, grid):
    slots = atoms[0].shape[1]
    return pl.pallas_call(
        functools.partial(interpolate_kernel, rows, grid, bits),
        out_shape=[jax.ShapeDtypeStruct((1, slots), jnp.float32)] * 3,
        in_specs=[smem()] * 2 + [vmem()] * 6,
        out_specs=[vmem()] * 3,
        scratch_shapes=[
            pltpu.VMEM((grid, GROUP), jnp.bfloat16),
            pltpu.VMEM((PAIR, 2 * grid, 2 * GROUP), jnp.bfloat16),
            pltpu.VMEM((PAIR, 8, GROUP), jnp.float32),
            pltpu.VMEM((PAIR, 8, GROUP), jnp.float32),
            pltpu.VMEM((PAIR, 24, GROUP), jnp.float32),
        ],
        cost_estimate=pl.CostEstimate(
            flops=STEP * rows * grid * slots * 12,
            bytes_accessed=planes * rows * grid * 4,
            transcendentals=0,
        ),
        name="interpolate",
    )(count, bounds, *atoms, tile)


def turns(grid, wave, place, quarter):
    whole = np.mod(wave * place + (grid // 4) * quarter, grid)
    return np.cos(2.0 * np.pi * whole / grid).astype(np.float32)


def wave_tables(grid, slabs, columns, waves):
    kx = np.arange(slabs * waves).reshape(slabs, 1, waves)
    part = np.arange(2)
    x = np.arange(grid)
    table_x = turns(grid, kx[None], x[:, None, None, None], part[None, None, :, None])
    kz = np.arange(grid).reshape(columns, 1, grid // columns, 1, 1)
    table_z = turns(
        grid, kz, x[None, None, None, :, None],
        part[None, :, None, None, None] - part[None, None, None, None, :],
    ).reshape(2 * grid, 2 * grid)
    y = np.arange(grid).reshape(columns, 1, grid // columns, 1, 1)
    table_y = turns(
        grid, x[None, None, None, None, :], y,
        part[None, None, None, :, None] - part[None, :, None, None, None],
    )
    return table_x, table_z, table_y


def signed_wave(waves, grid):
    return jnp.where(waves < grid // 2, waves, waves - grid)


def influence(moduli, screening, slab, column, grid, count_kx, count_kz):
    kx = slab * count_kx + lax.iota(jnp.int32, count_kx)
    kz = column * count_kz + lax.iota(jnp.int32, count_kz)
    ky = lax.iota(jnp.int32, grid)
    half = grid // 2
    share = jnp.where((kx == 0) | (kx == half), 1.0, 2.0)
    share = jnp.where(kx <= half, share, 0.0) * (0.5 * coulomb / grid**3)
    nx, nz, ny = (signed_wave(k, grid) for k in (kx, kz, ky))
    radius = (nz * nz)[:, None, None] + (nx * nx)[None, :, None] + (ny * ny)[None, None, :]
    squared = radius.astype(jnp.float32) / float(grid * grid)
    mirrored = jnp.roll(moduli[:, ::-1], 1, 1)
    spare = jnp.zeros((count_kx * lax.axis_size("gz"),), jnp.float32)

    def product(table):
        mx = lax.dynamic_slice_in_dim(
            jnp.concatenate([table[2], spare]), slab * count_kx, count_kx, 0
        )
        mz = lax.dynamic_slice_in_dim(table[0], column * count_kz, count_kz, 0)
        return mz[:, None, None] * (share * mx)[None, :, None] * table[1][None, None, :]

    both = product(moduli) + product(mirrored)
    safe = jnp.where(radius > 0, squared, 1.0)
    return jnp.where(radius > 0, both * jnp.exp(-screening[0] * squared) / safe, 0.0)


def exchange(x, axis):
    return lax.all_to_all(x, axis, split_axis=0, concat_axis=0, tiled=True)


def contract(form, *operands):
    return jnp.einsum(form, *operands, precision=high, preferred_element_type=jnp.float32)


def potential_field(block, kernel, tables, slabs, columns, waves):
    table_x, table_z, table_y = tables
    planes, rows, grid = block.shape
    lanes = waves * rows
    spectrum = contract("zyx,xpck->pzcky", block, table_x)
    spectrum = exchange(spectrum.reshape(slabs * planes * 2, lanes), "gz")
    spectrum = contract("mn,nl->ml", table_z, spectrum)
    spectrum = exchange(spectrum, "gy").reshape(columns, 2, grid // columns, waves, rows)
    spectrum = contract("pczky,pcydw->zkdw", spectrum, table_y)
    spectrum = spectrum * kernel[:, :, None, :]
    spectrum = contract("zkdw,pcydw->pczky", spectrum, table_y)
    spectrum = exchange(spectrum.reshape(2 * grid, lanes), "gy")
    spectrum = contract("mn,ml->nl", table_z, spectrum)
    spectrum = exchange(spectrum, "gz").reshape(slabs, planes, 2, waves, rows)
    return contract("pzcky,xpck->zyx", spectrum, table_x)


LANES = 128
MESH = pl.DeviceIdType.MESH


def fast_sizes(slabs, columns, planes, rows, grid):
    return (
        2 * rows == LANES
        and grid == 2 * LANES
        and columns * rows == grid
        and slabs * planes == grid
        and planes % 4 == 0
        and slabs >= 3
        and columns >= 3
    )


def green_rows(moduli, screening, slab, column, grid, count_kx, columns):
    half = grid // 2
    share_kz = half // columns
    kx = slab * count_kx + lax.iota(jnp.int32, count_kx)
    part = lax.broadcasted_iota(jnp.int32, (2, share_kz), 0)
    kz = part * half + column * share_kz + lax.broadcasted_iota(jnp.int32, (2, share_kz), 1)
    ky = lax.iota(jnp.int32, grid)
    share = jnp.where((kx == 0) | (kx == half), 1.0, 2.0)
    share = jnp.where(kx <= half, share, 0.0) * (0.5 * coulomb / grid**3)
    nx, nz, ny = (signed_wave(k, grid) for k in (kx, kz, ky))
    radius = (nx * nx)[:, None, None, None] + (nz * nz)[None, :, :, None] + (ny * ny)
    squared = radius.astype(jnp.float32) / float(grid * grid)
    mirrored = jnp.roll(moduli[:, ::-1], 1, 1)
    spare = jnp.zeros((count_kx * lax.axis_size("gz"),), jnp.float32)

    def product(table):
        mx = lax.dynamic_slice_in_dim(
            jnp.concatenate([table[2], spare]), slab * count_kx, count_kx, 0
        )
        mz = lax.dynamic_slice_in_dim(table[0].reshape(2, half), column * share_kz, share_kz, 1)
        return (share * mx)[:, None, None, None] * mz[None, :, :, None] * table[1]

    both = product(moduli) + product(mirrored)
    safe = jnp.where(radius > 0, squared, 1.0)
    green = jnp.where(radius > 0, both * jnp.exp(-screening[0] * squared) / safe, 0.0)
    return green.reshape(count_kx * grid // columns, grid)


def halves(table):
    table = np.ascontiguousarray(table, dtype=np.float32)
    top = table.astype(jnp.bfloat16)
    rest = (table - top.astype(np.float32)).astype(jnp.bfloat16)
    return top, rest


def solve_tables(grid, slabs, columns, waves, planes):
    half = grid // 2
    pairs = planes // 2
    share = half // columns
    x = np.arange(grid)
    part = np.arange(2)
    kx = np.repeat(np.arange(slabs * waves), 2)
    px = np.tile(part, slabs * waves)
    table_x = turns(grid, kx[:, None], x[None, :], px[:, None])
    top, rest = halves(table_x)
    forward_x = np.stack([top, rest])
    top, rest = halves(table_x.T)
    pad = round_up(3 * top.shape[1], LANES) - 3 * top.shape[1]
    inverse_x = np.concatenate([top, rest, top, np.zeros((grid, pad), top.dtype)], 1)
    kz = np.broadcast_to(np.arange(half).reshape(columns, 1, share), (columns, 2, share)).reshape(-1)
    pk = np.broadcast_to(part.reshape(1, 2, 1), (columns, 2, share)).reshape(-1)
    zh = np.broadcast_to(np.arange(half).reshape(slabs, 1, pairs), (slabs, 2, pairs)).reshape(-1)
    pz = np.broadcast_to(part.reshape(1, 2, 1), (slabs, 2, pairs)).reshape(-1)
    table_z = turns(half, kz[:, None], zh[None, :], pk[:, None] - pz[None, :])
    forward_z = np.stack(halves(table_z))
    inverse_z = np.stack(halves(table_z.T))
    ky = np.tile(np.arange(grid), 2)
    pf = np.repeat(part, grid)
    table_y = turns(grid, ky[:, None], ky[None, :], pf[None, :] - pf[:, None])
    forward_y = np.stack(halves(table_y))
    angle = 2.0 * np.pi * np.arange(half)[:, None] / grid
    upper = np.arange(LANES)[None, :] >= LANES // 2
    twist = np.stack(
        [np.where(upper, np.cos(angle), 1.0), np.where(upper, np.sin(angle), 0.0)]
    ).astype(np.float32)
    return forward_x, inverse_x, forward_z, inverse_z, forward_y, twist


def chunks_of(waves, count):
    edges = [waves * i // count for i in range(count + 1)]
    return [(a, b - a) for a, b in zip(edges, edges[1:]) if b > a]


def solve_kernel(
    slabs, columns, waves, planes, rows, grid, chunks,
    tile, green, table_fx, table_ix, table_fz, table_iz, table_y, twist, out,
    rim_z, rim_y, rim_c, block, fx, fz, iz, fy, iy,
    x_out, z_in, z_out, y_in, y_out, z_back, z_send, x_in, potential, y_left, y_right,
    rim_send, rim_recv, gz_send, gz_recv, gy_send, gy_recv, by_send, by_recv, bz_send, bz_recv,
):
    half = grid // 2
    pairs = planes // 2
    wide = 2 * pairs
    share = half // columns
    tall = 2 * share
    bins = 2 * slabs * waves
    slab = lax.axis_index("gz")
    column = lax.axis_index("gy")

    def around(step):
        return lax.rem(slab + step + slabs, slabs)

    def beside(step):
        return lax.rem(column + step + columns, columns)

    barrier = pltpu.get_barrier_semaphore()
    for step in range(1, slabs):
        pl.semaphore_signal(barrier, inc=1, device_id=(around(step), column), device_id_type=MESH)
    for step in range(1, columns):
        pl.semaphore_signal(barrier, inc=1, device_id=(slab, beside(step)), device_id_type=MESH)
    for step in (1, -1):
        pl.semaphore_signal(
            barrier, inc=1, device_id=(around(step), beside(step)), device_id_type=MESH
        )
    pl.semaphore_wait(barrier, slabs + columns)

    def remote(source, target, sends, recvs, at, to):
        return pltpu.make_async_remote_copy(
            src_ref=source, dst_ref=target, send_sem=sends.at[at], recv_sem=recvs.at[at],
            device_id=to, device_id_type=MESH,
        )

    main, edge = pl.ds(0, rows), pl.ds(rows, 8)
    body_z, over_z = pl.ds(0, planes), pl.ds(planes, 3)
    rims = [
        remote(tile.at[over_z, main], rim_z, rim_send, rim_recv, 0, (around(1), column)),
        remote(tile.at[body_z, edge], rim_y, rim_send, rim_recv, 1, (slab, beside(1))),
        remote(tile.at[over_z, edge], rim_c, rim_send, rim_recv, 2, (around(1), beside(1))),
    ]
    for copy in rims:
        copy.start()

    for source, target in ((table_fx, fx), (table_fz, fz), (table_iz, iz)):
        size = source.shape[2]
        target[:, :size] = source[0]
        target[:, size : 2 * size] = source[1]
        target[:, 2 * size :] = source[0]
    size = 2 * grid
    fy[:size, :] = table_y[0]
    fy[size : 2 * size, :] = table_y[0]
    fy[2 * size :, :] = table_y[1]
    iy[:, :size] = table_y[0]
    iy[:, size : 2 * size] = table_y[0]
    iy[:, 2 * size :] = table_y[1]
    potential[planes + 3 :] = jnp.zeros_like(potential[planes + 3 :])

    for copy in rims:
        copy.wait()

    def add_rims(at):
        block[pl.ds(at * 4, 4)] = tile[pl.ds(at * 4, 4), :rows, :]
        block[pl.ds(at * 4, 4), :8, :] += rim_y[pl.ds(at * 4, 4)]

    pl.loop(0, planes // 4)(add_rims)
    rim_z[:, :8, :] += rim_c[...]
    block[:3] += rim_z[...]

    def along_x(at):
        top, rest = split(block[pl.ds(at * 4, 4)].reshape(4 * rows, grid))
        values = lax.dot_general(
            fx[...], jnp.concatenate([top, top, rest], 1), (((1,), (1,)), ((), ())),
            preferred_element_type=jnp.float32,
        )
        for side in range(2):
            where = pl.ds(2 * at + side, bins, stride=pairs)
            x_out[where, :] = values[:, side * LANES : (side + 1) * LANES]

    pl.loop(0, planes // 4)(along_x)

    def gz_copy(q, step):
        w, n = chunks[q]
        source = x_out.at[pl.ds((around(step) * waves + w) * wide, n * wide)]
        target = z_in.at[slab, pl.ds(w * wide, n * wide)]
        return remote(source, target, gz_send, gz_recv, (q, step), (around(step), column))

    def gy_copy(q, step):
        w, n = chunks[q]
        where = pl.ds(w * tall, n * tall)
        source, target = z_out.at[beside(step), where], y_in.at[column, where]
        return remote(source, target, gy_send, gy_recv, (q, step), (slab, beside(step)))

    def by_copy(q, step):
        w, n = chunks[q]
        where = pl.ds(w * tall, n * tall)
        source, target = y_out.at[beside(step), where], z_back.at[column, where]
        return remote(source, target, by_send, by_recv, (q, step), (slab, beside(step)))

    def bz_copy(q, step):
        w, n = chunks[q]
        source = z_send.at[around(step), pl.ds(w * wide, n * wide)]
        target = x_in.at[pl.ds((slab * waves + w) * wide, n * wide)]
        return remote(source, target, bz_send, bz_recv, (q, step), (around(step), column))

    for q in range(len(chunks)):
        for step in range(1, slabs):
            gz_copy(q, step).start()
    z_in[slab] = x_out[pl.ds(pl.multiple_of(slab * waves * wide, wide), waves * wide), :]

    left = lax.broadcasted_iota(jnp.int32, (half, LANES), 1) < LANES // 2
    side = left[:share]

    def turn(value):
        return pltpu.roll(value, LANES // 2, 1)

    def three(value):
        top, rest = split(value)
        return jnp.concatenate([top, top, rest], 0)

    def to_z(q):
        for step in range(1, slabs):
            gz_copy(q, step).wait_recv()
        first, count = chunks[q]

        @pl.loop(first, first + count)
        def _(w):
            value = z_in[:, pl.ds(pl.multiple_of(w * wide, wide), wide), :].reshape(grid, LANES)
            value = jnp.dot(fz[...], three(value), preferred_element_type=jnp.float32)
            value = value.reshape(columns, 2, share, LANES)
            re = value[:, 0].reshape(half, LANES)
            im = value[:, 1].reshape(half, LANES)
            re, im = re * twist[0] + im * twist[1], im * twist[0] - re * twist[1]
            for p, v in enumerate((re, im)):
                v = jnp.where(left, v + turn(v), turn(v) - v)
                where = pl.ds(pl.multiple_of(w * tall + p * share, share), share)
                z_out[:, where, :] = v.reshape(columns, share, LANES)

        for step in range(1, columns):
            gy_copy(q, step).start()
        where = pl.ds(first * tall, count * tall)
        y_in[column, where, :] = z_out[column, where, :]

    def to_y(q):
        for step in range(1, columns):
            gy_copy(q, step).wait_recv()
        first, count = chunks[q]
        size = 2 * grid

        @pl.loop(0, count)
        def _(w):
            for p in range(2):
                where = pl.ds(pl.multiple_of((first + w) * tall + p * share, share), share)
                for c in range(0, columns, 2):
                    a, b = y_in[c, where, :], y_in[c + 1, where, :]
                    pair = (jnp.where(side, a, turn(b)), jnp.where(side, turn(a), b))
                    for h in range(2):
                        to = pl.ds(pl.multiple_of(w * tall + h * share, share), share)
                        at = (p * columns + c) * rows
                        top, rest = split(pair[h])
                        y_left[to, at : at + LANES] = top
                        y_left[to, size + at : size + at + LANES] = rest
                        y_left[to, 2 * size + at : 2 * size + at + LANES] = top

        value = jnp.dot(y_left[: count * tall, :], fy[...], preferred_element_type=jnp.float32)
        factor = green[first * tall : (first + count) * tall, :]
        value = jnp.concatenate([value[:, :grid] * factor, value[:, grid:] * factor], 1)
        top, rest = split(value)
        y_right[: count * tall, :] = lax.dot_general(
            jnp.concatenate([top, rest, top], 1), iy[...], (((1,), (1,)), ((), ())),
            preferred_element_type=jnp.float32,
        )

        @pl.loop(0, count)
        def _(w):
            for p in range(2):
                where = pl.ds(pl.multiple_of((first + w) * tall + p * share, share), share)
                for c in range(0, columns, 2):
                    at = (p * columns + c) * rows
                    a, b = (
                        y_right[
                            pl.ds(pl.multiple_of(w * tall + h * share, share), share),
                            at : at + LANES,
                        ]
                        for h in range(2)
                    )
                    y_out[c, where, :] = jnp.where(side, a, turn(b))
                    y_out[c + 1, where, :] = jnp.where(side, turn(a), b)

        for step in range(1, columns):
            by_copy(q, step).start()
        where = pl.ds(first * tall, count * tall)
        z_back[column, where, :] = y_out[column, where, :]

    def from_z(q):
        for step in range(1, columns):
            by_copy(q, step).wait_recv()
        first, count = chunks[q]

        @pl.loop(first, first + count)
        def _(w):
            value = z_back[:, pl.ds(pl.multiple_of(w * tall, tall), tall), :]
            re = value[:, :share].reshape(half, LANES)
            im = value[:, share:].reshape(half, LANES)
            re, im = (jnp.where(left, v + turn(v), turn(v) - v) for v in (re, im))
            re, im = re * twist[0] - im * twist[1], im * twist[0] + re * twist[1]
            re, im = (v.reshape(columns, share, LANES) for v in (re, im))
            value = jnp.concatenate(
                [v[c] for c in range(columns) for v in (re, im)], 0
            )
            value = jnp.dot(iz[...], three(value), preferred_element_type=jnp.float32)
            where = pl.ds(pl.multiple_of(w * wide, wide), wide)
            z_send[:, where, :] = value.reshape(slabs, wide, LANES)

        for step in range(1, slabs):
            bz_copy(q, step).start()
        where = pl.ds(pl.multiple_of((slab * waves + first) * wide, wide), count * wide)
        x_in[where, :] = z_send[slab, pl.ds(first * wide, count * wide), :]

    stages = (to_z, to_y, from_z)
    for turn_at in range(len(chunks) + len(stages) - 1):
        for at, stage in enumerate(stages):
            if 0 <= turn_at - at < len(chunks):
                stage(turn_at - at)
    for q in range(len(chunks)):
        for step in range(1, slabs):
            bz_copy(q, step).wait_recv()

    spare = table_ix.shape[1] - 3 * bins

    def back_x(at):
        value = jnp.concatenate(
            [x_in[pl.ds(2 * at + s, bins, stride=pairs), :] for s in range(2)], 1
        )
        top, rest = split(value)
        stack = [top, top, rest]
        if spare:
            stack.append(jnp.zeros((spare, 2 * LANES), jnp.bfloat16))
        value = jnp.dot(
            table_ix[...], jnp.concatenate(stack, 0), preferred_element_type=jnp.float32
        )
        potential[pl.ds(at * 4, 4), :rows, :] = value.T.reshape(4, rows, grid)

    pl.loop(0, planes // 4)(back_x)
    rims_back = [
        remote(
            potential.at[pl.ds(0, 3), main], potential.at[over_z, main],
            rim_send, rim_recv, 3, (around(-1), column),
        ),
        remote(
            potential.at[body_z, pl.ds(0, 8)], potential.at[body_z, edge],
            rim_send, rim_recv, 4, (slab, beside(-1)),
        ),
        remote(
            potential.at[pl.ds(0, 3), pl.ds(0, 8)], potential.at[over_z, edge],
            rim_send, rim_recv, 5, (around(-1), beside(-1)),
        ),
    ]
    for copy in rims_back:
        copy.start()
    for q in range(len(chunks)):
        for copy, steps in (
            (gz_copy, slabs), (gy_copy, columns), (by_copy, columns), (bz_copy, slabs)
        ):
            for step in range(1, steps):
                copy(q, step).wait_send()
    for copy in rims_back:
        copy.wait()

    def give(at):
        out[pl.ds(at * 4, 4)] = potential[pl.ds(at * 4, 4)]

    pl.loop(0, out.shape[0] // 4)(give)


def solve_fused(tile, green, slabs, columns, planes, rows, waves):
    span_planes, span_rows, grid = tile.shape
    tables = solve_tables(grid, slabs, columns, waves, planes)
    chunks = chunks_of(waves, CHUNKS)
    most = max(n for _, n in chunks)
    wide, tall = planes, 2 * (grid // 2 // columns)
    bins = 2 * slabs * waves

    def scratch(*shape):
        return pltpu.VMEM(shape, jnp.float32)

    def narrow(*shape):
        return pltpu.VMEM(shape, jnp.bfloat16)

    def flags(count):
        return [pltpu.SemaphoreType.DMA((len(chunks), count))] * 2

    return pl.pallas_call(
        functools.partial(
            solve_kernel, slabs, columns, waves, planes, rows, grid, chunks
        ),
        out_shape=jax.ShapeDtypeStruct(tile.shape, jnp.float32),
        in_specs=[vmem()] * 8,
        out_specs=vmem(),
        scratch_shapes=[
            scratch(3, rows, grid), scratch(planes, 8, grid), scratch(3, 8, grid),
            scratch(planes, rows, grid),
            narrow(bins, 3 * grid), narrow(grid, 3 * grid), narrow(grid, 3 * grid),
            narrow(6 * grid, 2 * grid), narrow(2 * grid, 6 * grid),
            scratch(slabs * waves * wide, LANES), scratch(slabs, waves * wide, LANES),
            scratch(columns, waves * tall, LANES), scratch(columns, waves * tall, LANES),
            scratch(columns, waves * tall, LANES), scratch(columns, waves * tall, LANES),
            scratch(slabs, waves * wide, LANES), scratch(slabs * waves * wide, LANES),
            scratch(*tile.shape),
            narrow(most * tall, 6 * grid), scratch(most * tall, 2 * grid),
            pltpu.SemaphoreType.DMA((6,)), pltpu.SemaphoreType.DMA((6,)),
            *flags(slabs), *flags(columns), *flags(columns), *flags(slabs),
        ],
        compiler_params=pltpu.CompilerParams(
            collective_id=0, has_side_effects=True, vmem_limit_bytes=60 * 1024 * 1024
        ),
        cost_estimate=pl.CostEstimate(
            flops=10**10, bytes_accessed=span_planes * span_rows * grid * 8, transcendentals=0
        ),
        name="solve",
    )(tile, green, *(jnp.asarray(t) for t in tables))


def solve_tile(volume, kernel, tables, planes, rows, waves, slabs, columns):
    span_planes, span_rows, grid = volume.shape
    rim_planes = shifted(volume[planes : planes + 3], "gz", 1)
    volume = jnp.concatenate([volume[:3] + rim_planes, volume[3:planes]], 0)
    rim_rows = shifted(volume[:, rows : rows + 3], "gy", 1)
    block = jnp.concatenate([volume[:, :3] + rim_rows, volume[:, 3:rows]], 1)
    potential = potential_field(block, kernel, tables, slabs, columns, waves)
    upper_rows = shifted(potential[:, :3], "gy", -1)
    spare_rows = jnp.zeros((planes, span_rows - rows - 3, grid), jnp.float32)
    widened = jnp.concatenate([potential, upper_rows, spare_rows], 1)
    upper_planes = shifted(widened[:3], "gz", -1)
    spare_planes = jnp.zeros((span_planes - planes - 3, span_rows, grid), jnp.float32)
    return jnp.concatenate([widened, upper_planes, spare_planes], 0)


def body(charge, fractions, cell_base, live_blocks, send_blocks, moduli, screening):
    slabs = lax.axis_size("gz")
    columns = lax.axis_size("gy")
    grid = moduli.shape[1]
    planes = grid // slabs
    rows = grid // columns
    span_planes = round_up(planes + 3 + STEP, 2)
    span_rows = round_up(rows + 3, 8)
    waves = -(-(grid // 2 + 1) // slabs)
    slab = lax.axis_index("gz")
    column = lax.axis_index("gy")
    lane_ids = lax.iota(jnp.int32, columns)
    live = jnp.sum(jnp.where(lane_ids == column, live_blocks[0], 0))
    send = jnp.sum(jnp.where(lane_ids == column, send_blocks[0], 0))
    kept_atoms = (live - send) * BLOCK
    live_atoms = live * BLOCK
    slots = charge.shape[0]
    bits = ((rows - 1).bit_length(), (grid - 1).bit_length())
    slot = lax.iota(jnp.int32, slots)
    key = jnp.where(slot < live_atoms, encode(cell_base, *bits), DEAD)
    key, slot, *values = lax.sort(
        (key, slot, charge, fractions[0], fractions[1], fractions[2]),
        num_keys=1, is_stable=False,
    )
    by_group = key.reshape(slots // GROUP, GROUP)
    alive = by_group < DEAD
    cell_z, cell_y, _ = decode(by_group, *bits)
    bounds = []
    for cell in (cell_z, cell_y):
        high = jnp.max(jnp.where(alive, cell, 0), 1)
        bounds += [jnp.min(jnp.where(alive, cell, high[:, None]), 1), high]
    bounds = jnp.stack(bounds)
    atoms = [v[None, :] for v in (key, *values)]
    sizes = (span_planes, span_rows, grid)
    count = live_atoms[None]
    tile = spread_atoms(count, bounds, atoms, bits, *sizes).reshape(sizes)
    if fast_sizes(slabs, columns, planes, rows, grid):
        green = green_rows(moduli, screening, slab, column, grid, waves, columns)
        padded = solve_fused(tile, green, slabs, columns, planes, rows, waves)
    else:
        tables = wave_tables(grid, slabs, columns, waves)
        kernel = influence(moduli, screening, slab, column, grid, waves, grid // columns)
        padded = solve_tile(tile, kernel, tables, planes, rows, waves, slabs, columns)
    padded = padded.reshape(span_planes * span_rows, grid)
    forces = interpolate_atoms(count, bounds, atoms, padded, bits, *sizes)
    _, *home = lax.sort((slot, *(f[0] for f in forces)), num_keys=1, is_stable=False)
    home = jnp.stack(home)
    margin = SEND_MAX * BLOCK
    room = jnp.concatenate([home, jnp.zeros((3, margin), jnp.float32)], 1)
    lent = lax.dynamic_slice_in_dim(room, kept_atoms, margin, 1)
    moved = shifted(lent, "gy", 1)
    kept = jnp.where(lax.iota(jnp.int32, slots) < kept_atoms, home, 0.0)
    holder = jnp.zeros((3, slots + margin), jnp.float32)
    holder = lax.dynamic_update_slice(holder, moved, (jnp.zeros((), jnp.int32), kept_atoms))
    return kept + holder[:, :slots]


def solution(mesh):
    return jax.shard_map(
        body,
        mesh=mesh,
        in_specs=(
            P(("gz", "gy")),
            P(None, ("gz", "gy")),
            P(None, ("gz", "gy")),
            P("gz", None),
            P("gz", None),
            P(),
            P(),
        ),
        out_specs=P(None, ("gz", "gy")),
        check_vma=False,
    )
```

```python
import functools

import jax
import jax.numpy as jnp
import numpy as np
from jax import lax
from jax.experimental import pallas as pl
from jax.experimental.pallas import tpu as pltpu
from jax.sharding import PartitionSpec as P

BLOCK = 128
SEND_MAX = 36
GROUP = 256
PAIR = 2
LAYER = 2
STEP = 7
WINDOW = 24
CHUNKS = 4
DEAD = 1 << 30

high = lax.Precision.HIGH
coulomb = 2.0


def shifted(x, axis, by):
    peers = lax.axis_size(axis)
    return lax.ppermute(x, axis, [(i, (i + by) % peers) for i in range(peers)])


def round_up(value, step):
    return -(-value // step) * step


def spline_weights(t):
    remain = 1.0 - t
    square = t * t
    cubed = square * t
    weights = [
        remain * remain * remain * (1.0 / 6.0),
        (3.0 * cubed - 6.0 * square + 4.0) * (1.0 / 6.0),
        (-3.0 * cubed + 3.0 * square + 3.0 * t + 1.0) * (1.0 / 6.0),
        cubed * (1.0 / 6.0),
    ]
    slopes = [
        -0.5 * remain * remain,
        1.5 * square - 2.0 * t,
        -1.5 * square + t + 0.5,
        0.5 * square,
    ]
    return weights, slopes


def stencil(base, weights, span):
    offset = lax.broadcasted_iota(jnp.int32, (span, base.shape[1]), 0) - base
    table = jnp.where(offset == 0, weights[0], 0.0)
    for k in range(1, 4):
        table = jnp.where(offset == k, weights[k], table)
    return table


def split(value):
    top = value.astype(jnp.bfloat16)
    rest = (value - top.astype(jnp.float32)).astype(jnp.bfloat16)
    return top, rest


def encode(cells, bits_y, bits_x):
    layer = cells[0] >> LAYER
    flip = (layer & 1) * ((1 << bits_y) - 1)
    inner = cells[0] & ((1 << LAYER) - 1)
    key = (layer << bits_y) | (cells[1] ^ flip)
    return (((key << LAYER) | inner) << bits_x) | cells[2]


def decode(key, bits_y, bits_x):
    inner = (key >> bits_x) & ((1 << LAYER) - 1)
    y = (key >> (bits_x + LAYER)) & ((1 << bits_y) - 1)
    layer = key >> (bits_x + LAYER + bits_y)
    y = y ^ ((layer & 1) * ((1 << bits_y) - 1))
    return (layer << LAYER) | inner, y, key & ((1 << bits_x) - 1)


def wrapped_stencil(places, base, weights, grid):
    top_table = rest_table = jnp.zeros(places.shape, jnp.bfloat16)
    for k in range(4):
        at = base + k
        at = jnp.where(at >= grid, at - grid, at).astype(jnp.float32).astype(jnp.bfloat16)
        hit = places == at
        top, rest = split(weights[k])
        top_table = jnp.where(hit, top, top_table)
        rest_table = jnp.where(hit, rest, rest_table)
    return top_table, rest_table


def fill_places(places):
    places[...] = (
        lax.broadcasted_iota(jnp.int32, places.shape, 0).astype(jnp.float32).astype(jnp.bfloat16)
    )


def over_windows(bounds, group, visit):
    low_z, high_z, low_y, high_y = (bound[group] for bound in bounds)
    start = (low_y // 8) * 8
    steps = (high_z + 3 - low_z) // STEP + 1
    strips = (high_y + 3 - start) // WINDOW + 1
    visit(low_z, start)

    def rest():
        @pl.loop(1, steps * strips)
        def _(at):
            visit(low_z + lax.rem(at, steps) * STEP, start + lax.div(at, steps) * WINDOW)

    return rest


def over_groups(atoms, prepare):
    @pl.loop(0, (atoms + PAIR * GROUP - 1) // (PAIR * GROUP))
    def _(turn):
        later = [prepare(turn * PAIR + i, i) for i in range(PAIR)]
        for rest in later:
            rest()


def spread_kernel(
    rows, grid, bits, count, low_z, high_z, low_y, high_y, key, charge, fz, fy, fx, tile, places, table_z, factor_x,
):
    tile[...] = jnp.zeros_like(tile)
    fill_places(places)
    atoms = count[0]

    def prepare(group, lane):
        at = pl.ds(pl.multiple_of(group * GROUP, GROUP), GROUP)
        place = group * GROUP + lax.broadcasted_iota(jnp.int32, (1, GROUP), 1)
        value = jnp.where(place < atoms, charge[0:1, at], 0.0)
        cell_z, cell_y, cell_x = decode(key[0:1, at], *bits)
        weight_z, _ = spline_weights(fz[0:1, at])
        weight_y, _ = spline_weights(fy[0:1, at])
        weight_x, _ = spline_weights(fx[0:1, at])
        weight_x = [value * w for w in weight_x]
        top, rest = wrapped_stencil(places[...], cell_x, weight_x, grid)
        factor_x[lane, :, :GROUP] = top
        factor_x[lane, :, GROUP:] = rest

        def visit(first, start):
            table_z[lane] = stencil(cell_z - first, weight_z, table_z.shape[1])
            table_y = stencil(cell_y - start, weight_y, WINDOW)
            part = jnp.concatenate([table_z[lane, j : j + 1, :] * table_y for j in range(STEP)], 0)
            top, rest = split(part)
            across = (((1,), (1,)), ((), ()))
            values = lax.dot_general(
                jnp.concatenate([top, rest], 0), factor_x[lane, :, :GROUP], across,
                preferred_element_type=jnp.float32,
            )
            values = values[: STEP * WINDOW] + values[STEP * WINDOW :] + lax.dot_general(
                top, factor_x[lane, :, GROUP:], across, preferred_element_type=jnp.float32
            )
            for j in range(STEP):
                where = pl.ds(pl.multiple_of((first + j) * rows + start, 8), WINDOW)
                tile[where, :] += values[j * WINDOW : (j + 1) * WINDOW, :]

        return over_windows((low_z, high_z, low_y, high_y), group, visit)

    over_groups(atoms, prepare)


def interpolate_kernel(
    rows, grid, bits, count, low_z, high_z, low_y, high_y, key, charge, fz, fy, fx, tile, force_z, force_y, force_x,
    places, factor_x, table_z, rising_z, total,
):
    force_z[...] = jnp.zeros_like(force_z)
    force_y[...] = jnp.zeros_like(force_y)
    force_x[...] = jnp.zeros_like(force_x)
    fill_places(places)
    atoms = count[0]

    def prepare(group, lane):
        at = pl.ds(pl.multiple_of(group * GROUP, GROUP), GROUP)
        place = group * GROUP + lax.broadcasted_iota(jnp.int32, (1, GROUP), 1)
        value = -jnp.where(place < atoms, charge[0:1, at], 0.0)
        cell_z, cell_y, cell_x = decode(key[0:1, at], *bits)
        weight_z, slope_z = spline_weights(fz[0:1, at])
        weight_y, slope_y = spline_weights(fy[0:1, at])
        weight_x, slope_x = spline_weights(fx[0:1, at])
        for half, values in enumerate((weight_x, slope_x)):
            top, rest = wrapped_stencil(places[...], cell_x, values, grid)
            columns = slice(half * GROUP, (half + 1) * GROUP)
            factor_x[lane, :grid, columns] = top
            factor_x[lane, grid:, columns] = rest
        total[lane] = jnp.zeros(total.shape[1:], jnp.float32)

        def visit(first, start):
            span = table_z.shape[1]
            table_z[lane] = stencil(cell_z - first, weight_z, span)
            rising_z[lane] = stencil(cell_z - first, slope_z, span)
            top, rest = split(
                jnp.concatenate(
                    [
                        tile[pl.ds(pl.multiple_of((first + j) * rows + start, 8), WINDOW), :]
                        for j in range(STEP)
                    ],
                    0,
                )
            )
            along = jnp.dot(
                jnp.concatenate([top, rest], 0), factor_x[lane, :grid, :],
                preferred_element_type=jnp.float32,
            )
            along = along[: STEP * WINDOW] + along[STEP * WINDOW :] + jnp.dot(
                top, factor_x[lane, grid:, :], preferred_element_type=jnp.float32
            )
            table_y = stencil(cell_y - start, weight_y, WINDOW)
            rising_y = stencil(cell_y - start, slope_y, WINDOW)
            zs = [table_z[lane, j : j + 1, :] for j in range(STEP)]
            gs = [rising_z[lane, j : j + 1, :] for j in range(STEP)]
            sums = [0.0, 0.0, 0.0]
            for r in range(0, WINDOW, 8):
                local = slice(r, r + 8)
                w = [along[j * WINDOW + r : j * WINDOW + r + 8, :GROUP] for j in range(STEP)]
                s = [along[j * WINDOW + r : j * WINDOW + r + 8, GROUP:] for j in range(STEP)]
                sums[0] += table_y[local] * sum(gs[j] * w[j] for j in range(STEP))
                sums[1] += rising_y[local] * sum(zs[j] * w[j] for j in range(STEP))
                sums[2] += table_y[local] * sum(zs[j] * s[j] for j in range(STEP))
            for i in range(3):
                total[lane, 8 * i : 8 * i + 8, :] += sums[i]

        rest_of = over_windows((low_z, high_z, low_y, high_y), group, visit)

        def finish():
            rest_of()
            for i, force in enumerate((force_z, force_y, force_x)):
                part = total[lane, 8 * i : 8 * i + 8, :]
                force[0:1, at] = value * jnp.sum(part, 0, keepdims=True)

        return finish

    over_groups(atoms, prepare)


def vmem():
    return pl.BlockSpec(memory_space=pltpu.VMEM)


def smem():
    return pl.BlockSpec(memory_space=pltpu.SMEM)


def spread_atoms(count, bounds, atoms, bits, planes, rows, grid):
    slots = atoms[0].shape[1]
    return pl.pallas_call(
        functools.partial(spread_kernel, rows, grid, bits),
        out_shape=jax.ShapeDtypeStruct((planes * rows, grid), jnp.float32),
        in_specs=[smem()] * 5 + [vmem()] * 5,
        out_specs=vmem(),
        scratch_shapes=[
            pltpu.VMEM((grid, GROUP), jnp.bfloat16),
            pltpu.VMEM((PAIR, 8, GROUP), jnp.float32),
            pltpu.VMEM((PAIR, grid, 2 * GROUP), jnp.bfloat16),
        ],
        cost_estimate=pl.CostEstimate(
            flops=STEP * rows * grid * slots * 6,
            bytes_accessed=planes * rows * grid * 4,
            transcendentals=0,
        ),
        name="spread",
    )(count, *bounds, *atoms)


def interpolate_atoms(count, bounds, atoms, tile, bits, planes, rows, grid):
    slots = atoms[0].shape[1]
    return pl.pallas_call(
        functools.partial(interpolate_kernel, rows, grid, bits),
        out_shape=[jax.ShapeDtypeStruct((1, slots), jnp.float32)] * 3,
        in_specs=[smem()] * 5 + [vmem()] * 6,
        out_specs=[vmem()] * 3,
        scratch_shapes=[
            pltpu.VMEM((grid, GROUP), jnp.bfloat16),
            pltpu.VMEM((PAIR, 2 * grid, 2 * GROUP), jnp.bfloat16),
            pltpu.VMEM((PAIR, 8, GROUP), jnp.float32),
            pltpu.VMEM((PAIR, 8, GROUP), jnp.float32),
            pltpu.VMEM((PAIR, 24, GROUP), jnp.float32),
        ],
        cost_estimate=pl.CostEstimate(
            flops=STEP * rows * grid * slots * 12,
            bytes_accessed=planes * rows * grid * 4,
            transcendentals=0,
        ),
        name="interpolate",
    )(count, *bounds, *atoms, tile)


def turns(grid, wave, place, quarter):
    whole = np.mod(wave * place + (grid // 4) * quarter, grid)
    return np.cos(2.0 * np.pi * whole / grid).astype(np.float32)


def wave_tables(grid, slabs, columns, waves):
    kx = np.arange(slabs * waves).reshape(slabs, 1, waves)
    part = np.arange(2)
    x = np.arange(grid)
    table_x = turns(grid, kx[None], x[:, None, None, None], part[None, None, :, None])
    kz = np.arange(grid).reshape(columns, 1, grid // columns, 1, 1)
    table_z = turns(
        grid, kz, x[None, None, None, :, None],
        part[None, :, None, None, None] - part[None, None, None, None, :],
    ).reshape(2 * grid, 2 * grid)
    y = np.arange(grid).reshape(columns, 1, grid // columns, 1, 1)
    table_y = turns(
        grid, x[None, None, None, None, :], y,
        part[None, None, None, :, None] - part[None, :, None, None, None],
    )
    return table_x, table_z, table_y


def signed_wave(waves, grid):
    return jnp.where(waves < grid // 2, waves, waves - grid)


def influence(moduli, screening, slab, column, grid, count_kx, count_kz):
    kx = slab * count_kx + lax.iota(jnp.int32, count_kx)
    kz = column * count_kz + lax.iota(jnp.int32, count_kz)
    ky = lax.iota(jnp.int32, grid)
    half = grid // 2
    share = jnp.where((kx == 0) | (kx == half), 1.0, 2.0)
    share = jnp.where(kx <= half, share, 0.0) * (0.5 * coulomb / grid**3)
    nx, nz, ny = (signed_wave(k, grid) for k in (kx, kz, ky))
    radius = (nz * nz)[:, None, None] + (nx * nx)[None, :, None] + (ny * ny)[None, None, :]
    squared = radius.astype(jnp.float32) / float(grid * grid)
    mirrored = jnp.roll(moduli[:, ::-1], 1, 1)
    spare = jnp.zeros((count_kx * lax.axis_size("gz"),), jnp.float32)

    def product(table):
        mx = lax.dynamic_slice_in_dim(
            jnp.concatenate([table[2], spare]), slab * count_kx, count_kx, 0
        )
        mz = lax.dynamic_slice_in_dim(table[0], column * count_kz, count_kz, 0)
        return mz[:, None, None] * (share * mx)[None, :, None] * table[1][None, None, :]

    both = product(moduli) + product(mirrored)
    safe = jnp.where(radius > 0, squared, 1.0)
    return jnp.where(radius > 0, both * jnp.exp(-screening[0] * squared) / safe, 0.0)


def exchange(x, axis):
    return lax.all_to_all(x, axis, split_axis=0, concat_axis=0, tiled=True)


def contract(form, *operands):
    return jnp.einsum(form, *operands, precision=high, preferred_element_type=jnp.float32)


def potential_field(block, kernel, tables, slabs, columns, waves):
    table_x, table_z, table_y = tables
    planes, rows, grid = block.shape
    lanes = waves * rows
    spectrum = contract("zyx,xpck->pzcky", block, table_x)
    spectrum = exchange(spectrum.reshape(slabs * planes * 2, lanes), "gz")
    spectrum = contract("mn,nl->ml", table_z, spectrum)
    spectrum = exchange(spectrum, "gy").reshape(columns, 2, grid // columns, waves, rows)
    spectrum = contract("pczky,pcydw->zkdw", spectrum, table_y)
    spectrum = spectrum * kernel[:, :, None, :]
    spectrum = contract("zkdw,pcydw->pczky", spectrum, table_y)
    spectrum = exchange(spectrum.reshape(2 * grid, lanes), "gy")
    spectrum = contract("mn,ml->nl", table_z, spectrum)
    spectrum = exchange(spectrum, "gz").reshape(slabs, planes, 2, waves, rows)
    return contract("pzcky,xpck->zyx", spectrum, table_x)


LANES = 128
MESH = pl.DeviceIdType.MESH


def fast_sizes(slabs, columns, planes, rows, grid):
    return (
        2 * rows == LANES
        and grid == 2 * LANES
        and columns * rows == grid
        and slabs * planes == grid
        and planes % 8 == 0
        and LANES % (2 * columns) == 0
        and LANES % slabs == 0
        and slabs >= 3
        and columns >= 3
    )


def kept_waves(half, columns):
    pairs = [k for n in range(1, half // 2) for k in (n, half - n)]
    return np.array([0, half // 2] + pairs).reshape(columns, half // columns)


def partners(half, columns):
    share = half // columns
    moves = np.zeros((columns, 2 * share, 2 * share), np.float32)
    for c, waves in enumerate(kept_waves(half, columns)):
        place = {int(k): j for j, k in enumerate(waves)}
        for h in range(2):
            for k, j in place.items():
                other = (2 * half - h * half - k) % (2 * half)
                moves[c, h * share + j, other // half * share + place[other % half]] = 1.0
    return moves.astype(jnp.bfloat16)


def fill_green(green, moduli, screening, slab, column, waves, columns):
    grid = moduli.shape[1]
    half = grid // 2
    share = half // columns
    tall = 2 * share

    def signed(k):
        return jnp.where(k < half, k, k - grid)

    def opposite(k):
        return jnp.where(k == 0, 0, grid - k)

    def pick(lanes, at, values):
        return jnp.sum(jnp.where(lanes == at, values, 0.0), 1, keepdims=True)

    down = lax.broadcasted_iota(jnp.int32, (grid, grid), 0)
    over = lax.broadcasted_iota(jnp.int32, (grid, grid), 1)
    turned = pick(over, opposite(down), moduli[1:2, :])
    factor_y = moduli[1:2, :]
    mirror_y = jnp.sum(jnp.where(down == over, turned, 0.0), 0, keepdims=True)
    lanes = over[:tall]
    row = down[:tall]
    upper = jnp.where(row >= share, 1, 0)
    place = column * share + row - upper * share
    kept = jnp.where((place & 1) == 0, place >> 1, half - (place >> 1))
    kz = upper * half + jnp.where(place == 1, half // 2, kept)
    factor_z = pick(lanes, kz, moduli[0:1, :])
    mirror_z = pick(lanes, opposite(kz), moduli[0:1, :])
    flat = signed(kz) * signed(kz) + signed(lanes) * signed(lanes)

    def values(kx):
        share_x = jnp.where((kx == 0) | (kx == half), 1.0, 2.0) * (0.5 * coulomb / grid**3)
        factor_x = share_x * pick(over[:1], kx, moduli[2:3, :])
        mirror_x = share_x * pick(over[:1], opposite(kx), moduli[2:3, :])
        both = factor_x * factor_z * factor_y + mirror_x * mirror_z * mirror_y
        radius = flat + signed(kx) * signed(kx)
        squared = radius.astype(jnp.float32) * (1.0 / (grid * grid))
        safe = jnp.where(radius > 0, squared, 1.0)
        return jnp.where(radius > 0, both * jnp.exp(-screening[0] * squared) / safe, 0.0)

    plain = values(slab * waves)
    ends = values(half)
    green[:tall, :] = jnp.where(slab == 0, 0.5 * (plain + ends), plain)
    green[waves * tall :, :] = jnp.where(slab == 0, 0.5 * (plain - ends), 0.0)

    @pl.loop(1, waves)
    def _(w):
        green[pl.ds(pl.multiple_of(w * tall, tall), tall), :] = values(slab * waves + w)


def halves(table):
    table = np.ascontiguousarray(table, dtype=np.float32)
    top = table.astype(jnp.bfloat16)
    rest = (table - top.astype(np.float32)).astype(jnp.bfloat16)
    return top, rest


def solve_tables(grid, slabs, columns, waves, planes):
    half = grid // 2
    pairs = planes // 2
    share = half // columns
    x = np.arange(grid)
    part = np.arange(2)
    kx = np.repeat(np.arange(slabs * waves), 2)
    px = np.tile(part, slabs * waves)
    table_x = turns(grid, kx[:, None], x[None, :], px[:, None])
    table_x[1] = np.where(x % 2, -1.0, 1.0)
    forward_x = np.concatenate(halves(table_x))
    inverse_x = np.concatenate(halves(table_x.T))
    kept = kept_waves(half, columns)
    kz = np.broadcast_to(kept[:, None, :], (columns, 2, share)).reshape(-1)
    pk = np.broadcast_to(part.reshape(1, 2, 1), (columns, 2, share)).reshape(-1)
    zh = np.broadcast_to(np.arange(half).reshape(slabs, 1, pairs), (slabs, 2, pairs)).reshape(-1)
    pz = np.broadcast_to(part.reshape(1, 2, 1), (slabs, 2, pairs)).reshape(-1)
    table_z = turns(half, kz[:, None], zh[None, :], pk[:, None] - pz[None, :])
    forward_z = np.stack(halves(table_z))
    inverse_z = np.stack(halves(table_z.T))
    ky = np.tile(np.arange(grid), 2)
    pf = np.repeat(part, grid)
    table_y = turns(grid, ky[:, None], ky[None, :], pf[None, :] - pf[:, None])
    forward_y = np.stack(halves(table_y))
    angle = 2.0 * np.pi * kept.reshape(-1, 1) / grid
    upper = np.arange(LANES)[None, :] >= LANES // 2
    twist = np.stack(
        [np.where(upper, np.cos(angle), 1.0), np.where(upper, np.sin(angle), 0.0)]
    ).astype(np.float32)
    return forward_x, inverse_x, forward_z, inverse_z, forward_y, twist, partners(half, columns)


def chunks_of(waves, count):
    edges = [waves * i // count for i in range(count + 1)]
    return [(a, b - a) for a, b in zip(edges, edges[1:]) if b > a]


def solve_kernel(
    slabs, columns, waves, planes, rows, grid, chunks,
    tile, moduli, screening, table_fx, table_ix, table_fz, table_iz, table_y, twist, moves, out,
    green, rim_z, rim_y, rim_c,
    x_out, z_in, z_out, y_in, y_out, z_back, z_send, x_in, y_top, y_rest, y_right,
    rim_send, rim_recv, gz_send, gz_recv, gy_send, gy_recv, by_send, by_recv, bz_send, bz_recv,
):
    half = grid // 2
    pairs = planes // 2
    wide = 2 * pairs
    share = half // columns
    tall = 2 * share
    bins = 2 * slabs * waves
    slab = lax.axis_index("gz")
    column = lax.axis_index("gy")

    def around(step):
        return lax.rem(slab + step + slabs, slabs)

    def beside(step):
        return lax.rem(column + step + columns, columns)

    barrier = pltpu.get_barrier_semaphore()
    for step in range(1, slabs):
        pl.semaphore_signal(barrier, inc=1, device_id=(around(step), column), device_id_type=MESH)
    for step in range(1, columns):
        pl.semaphore_signal(barrier, inc=1, device_id=(slab, beside(step)), device_id_type=MESH)
    for step in (1, -1):
        pl.semaphore_signal(
            barrier, inc=1, device_id=(around(step), beside(step)), device_id_type=MESH
        )
    pl.semaphore_wait(barrier, slabs + columns)

    def remote(source, target, sends, recvs, at, to):
        return pltpu.make_async_remote_copy(
            src_ref=source, dst_ref=target, send_sem=sends.at[at], recv_sem=recvs.at[at],
            device_id=to, device_id_type=MESH,
        )

    main, edge = pl.ds(0, rows), pl.ds(rows, 8)
    body_z, over_z = pl.ds(0, planes), pl.ds(planes, 3)
    rims = [
        remote(tile.at[over_z, main], rim_z, rim_send, rim_recv, 0, (around(1), column)),
        remote(tile.at[body_z, edge], rim_y, rim_send, rim_recv, 1, (slab, beside(1))),
        remote(tile.at[over_z, edge], rim_c, rim_send, rim_recv, 2, (around(1), beside(1))),
    ]
    for copy in rims:
        copy.start()

    out[planes + 3 :] = jnp.zeros_like(out[planes + 3 :])
    across = (((1,), (1,)), ((), ()))

    def product(left, right, form=(((1,), (0,)), ((), ()))):
        return lax.dot_general(left, right, form, preferred_element_type=jnp.float32)

    def along_x(at, rim):
        value = tile[pl.ds(at * 4, 4), :rows, :]
        head = value[:, :8] + rim_y[pl.ds(at * 4, 4)]
        value = jnp.concatenate([head, value[:, 8:]], 1)
        if rim is not None:
            value = value + jnp.concatenate([rim, jnp.zeros((1, rows, grid), jnp.float32)], 0)
        top, rest = split(value.reshape(4 * rows, grid))
        both = product(table_fx[...], top, across)
        values = both[:bins] + both[bins:] + product(table_fx[:bins, :], rest, across)
        for side in range(2):
            where = pl.ds(2 * at + side, bins, stride=pairs)
            x_out[where, :] = values[:, side * LANES : (side + 1) * LANES]

    rims[1].wait()

    @pl.loop(0, (planes // 4 - 2) // 2)
    def _(turn_at):
        along_x(2 * turn_at + 1, None)
        along_x(2 * turn_at + 2, None)

    rims[0].wait()
    rims[2].wait()
    rim_z[:, :8, :] += rim_c[...]
    along_x(planes // 4 - 1, None)
    along_x(0, rim_z[...])

    def gz_copy(q, step):
        w, n = chunks[q]
        source = x_out.at[pl.ds((around(step) * waves + w) * wide, n * wide)]
        target = z_in.at[slab, pl.ds(w * wide, n * wide)]
        return remote(source, target, gz_send, gz_recv, (q, step), (around(step), column))

    def gy_copy(q, step):
        w, n = chunks[q]
        where = pl.ds(w * tall, n * tall)
        source, target = z_out.at[beside(step), where], y_in.at[column, where]
        return remote(source, target, gy_send, gy_recv, (q, step), (slab, beside(step)))

    def by_copy(q, step):
        w, n = chunks[q]
        where = pl.ds(w * tall, n * tall)
        source, target = y_out.at[beside(step), where], z_back.at[column, where]
        return remote(source, target, by_send, by_recv, (q, step), (slab, beside(step)))

    def bz_copy(q, step):
        w, n = chunks[q]
        source = z_send.at[around(step), pl.ds(w * wide, n * wide)]
        target = x_in.at[pl.ds((slab * waves + w) * wide, n * wide)]
        return remote(source, target, bz_send, bz_recv, (q, step), (around(step), column))

    for q in range(len(chunks)):
        for step in range(1, slabs):
            gz_copy(q, step).start()
    z_in[slab] = x_out[pl.ds(pl.multiple_of(slab * waves * wide, wide), waves * wide), :]

    fill_green(green, moduli, screening, slab, column, waves, columns)
    left = lax.broadcasted_iota(jnp.int32, (half, LANES), 1) < LANES // 2
    side = left[:share]

    def turn(value):
        return pltpu.roll(value, LANES // 2, 1)

    def along_z(table, value):
        top, rest = split(value)
        both = product(table[0], jnp.concatenate([top, rest], 1))
        return both[:, :LANES] + both[:, LANES:] + product(table[1], top)

    def to_z(q):
        for step in range(1, slabs):
            gz_copy(q, step).wait_recv()
        first, count = chunks[q]

        @pl.loop(first, first + count)
        def _(w):
            value = z_in[:, pl.ds(pl.multiple_of(w * wide, wide), wide), :].reshape(grid, LANES)
            value = along_z(table_fz, value)
            value = value.reshape(columns, 2, share, LANES)
            re = value[:, 0].reshape(half, LANES)
            im = value[:, 1].reshape(half, LANES)
            re, im = re * twist[0] + im * twist[1], im * twist[0] - re * twist[1]
            for p, v in enumerate((re, im)):
                v = jnp.where(left, v + turn(v), turn(v) - v)
                where = pl.ds(pl.multiple_of(w * tall + p * share, share), share)
                z_out[:, where, :] = v.reshape(columns, share, LANES)

        for step in range(1, columns):
            gy_copy(q, step).start()
        where = pl.ds(first * tall, count * tall)
        y_in[column, where, :] = z_out[column, where, :]

    def to_y(q):
        for step in range(1, columns):
            gy_copy(q, step).wait_recv()
        first, count = chunks[q]

        @pl.loop(0, count)
        def _(w):
            for p in range(2):
                where = pl.ds(pl.multiple_of((first + w) * tall + p * share, share), share)
                for c in range(0, columns, 2):
                    a, b = y_in[c, where, :], y_in[c + 1, where, :]
                    pair = (jnp.where(side, a, turn(b)), jnp.where(side, turn(a), b))
                    for h in range(2):
                        to = pl.ds(pl.multiple_of(w * tall + h * share, share), share)
                        at = (p * columns + c) * rows
                        top, rest = split(pair[h])
                        y_top[to, at : at + LANES] = top
                        y_rest[to, at : at + LANES] = rest

        main_rows = size = count * tall
        if first == 0:
            size += tall
            for target in (y_top, y_rest):
                value = product(moves[column], target[:tall, :])
                value = jnp.concatenate([value[:, :grid], -value[:, grid:]], 1)
                target[main_rows:size, :] = value.astype(jnp.bfloat16)
        top = y_top[:size, :]
        both = product(jnp.concatenate([top, y_rest[:size, :]], 0), table_y[0])
        value = both[:size] + both[size:] + product(top, table_y[1])
        factor = green[first * tall : (first + count) * tall, :]
        if first == 0:
            factor = jnp.concatenate([factor, green[waves * tall :, :]], 0)
        value = jnp.concatenate([value[:, :grid] * factor, value[:, grid:] * factor], 1)
        if first == 0:
            value = jnp.concatenate([value[:tall] + value[main_rows:], value[tall:main_rows]], 0)
        size = main_rows
        top, rest = split(value)
        both = product(jnp.concatenate([top, rest], 0), table_y[0], across)
        y_right[:size, :] = both[:size] + both[size:] + product(top, table_y[1], across)

        @pl.loop(0, count)
        def _(w):
            for p in range(2):
                where = pl.ds(pl.multiple_of((first + w) * tall + p * share, share), share)
                for c in range(0, columns, 2):
                    at = (p * columns + c) * rows
                    a, b = (
                        y_right[
                            pl.ds(pl.multiple_of(w * tall + h * share, share), share),
                            at : at + LANES,
                        ]
                        for h in range(2)
                    )
                    y_out[c, where, :] = jnp.where(side, a, turn(b))
                    y_out[c + 1, where, :] = jnp.where(side, turn(a), b)

        for step in range(1, columns):
            by_copy(q, step).start()
        where = pl.ds(first * tall, count * tall)
        z_back[column, where, :] = y_out[column, where, :]

    def from_z(q):
        for step in range(1, columns):
            by_copy(q, step).wait_recv()
        first, count = chunks[q]

        @pl.loop(first, first + count)
        def _(w):
            value = z_back[:, pl.ds(pl.multiple_of(w * tall, tall), tall), :]
            re = value[:, :share].reshape(half, LANES)
            im = value[:, share:].reshape(half, LANES)
            re, im = (jnp.where(left, v + turn(v), turn(v) - v) for v in (re, im))
            re, im = re * twist[0] - im * twist[1], im * twist[0] + re * twist[1]
            re, im = (v.reshape(columns, share, LANES) for v in (re, im))
            value = jnp.concatenate(
                [v[c] for c in range(columns) for v in (re, im)], 0
            )
            value = along_z(table_iz, value)
            where = pl.ds(pl.multiple_of(w * wide, wide), wide)
            z_send[:, where, :] = value.reshape(slabs, wide, LANES)

        for step in range(1, slabs):
            bz_copy(q, step).start()
        where = pl.ds(pl.multiple_of((slab * waves + first) * wide, wide), count * wide)
        x_in[where, :] = z_send[slab, pl.ds(first * wide, count * wide), :]

    stages = (to_z, to_y, from_z)
    for turn_at in range(len(chunks) + len(stages) - 1):
        for at, stage in enumerate(stages):
            if 0 <= turn_at - at < len(chunks):
                stage(turn_at - at)
    for q in range(len(chunks)):
        for step in range(1, slabs):
            bz_copy(q, step).wait_recv()

    def back_x(at):
        value = jnp.concatenate(
            [x_in[pl.ds(2 * at + s, bins, stride=pairs), :] for s in range(2)], 1
        )
        top, rest = split(value)
        both = product(table_ix[...], top)
        value = both[:grid] + both[grid:] + product(table_ix[:grid, :], rest)
        out[pl.ds(at * 4, 4), :rows, :] = value.T.reshape(4, rows, grid)

    def rim_back(at):
        planes_of = pl.ds(8 * at, 8)
        return remote(
            out.at[planes_of, pl.ds(0, 8)], out.at[planes_of, edge],
            rim_send, rim_recv, 5 + at, (slab, beside(-1)),
        )

    rims_back = [rim_back(at) for at in range(planes // 8)] + [
        remote(
            out.at[pl.ds(0, 3), main], out.at[over_z, main],
            rim_send, rim_recv, 3, (around(-1), column),
        ),
        remote(
            out.at[pl.ds(0, 3), pl.ds(0, 8)], out.at[over_z, edge],
            rim_send, rim_recv, 4, (around(-1), beside(-1)),
        ),
    ]
    for at in range(planes // 8):
        back_x(2 * at)
        back_x(2 * at + 1)
        if at == 1:
            for copy in rims_back[-2:]:
                copy.start()
        if at > 0:
            rims_back[at - 1].start()
    rims_back[planes // 8 - 1].start()
    for q in range(len(chunks)):
        for copy, steps in (
            (gz_copy, slabs), (gy_copy, columns), (by_copy, columns), (bz_copy, slabs)
        ):
            for step in range(1, steps):
                copy(q, step).wait_send()
    for copy in rims_back:
        copy.wait()


def solve_fused(tile, moduli, screening, slabs, columns, planes, rows, waves):
    span_planes, span_rows, grid = tile.shape
    tables = solve_tables(grid, slabs, columns, waves, planes)
    chunks = chunks_of(waves, CHUNKS)
    most = max(n for _, n in chunks)
    wide, tall = planes, 2 * (grid // 2 // columns)

    def scratch(*shape):
        return pltpu.VMEM(shape, jnp.float32)

    def narrow(*shape):
        return pltpu.VMEM(shape, jnp.bfloat16)

    def flags(count):
        return [pltpu.SemaphoreType.DMA((len(chunks), count))] * 2

    return pl.pallas_call(
        functools.partial(
            solve_kernel, slabs, columns, waves, planes, rows, grid, chunks
        ),
        out_shape=jax.ShapeDtypeStruct(tile.shape, jnp.float32),
        in_specs=[vmem()] * 2 + [smem()] + [vmem()] * 7,
        out_specs=vmem(),
        scratch_shapes=[
            scratch((waves + 1) * tall, grid),
            scratch(3, rows, grid), scratch(planes, 8, grid), scratch(3, 8, grid),
            scratch(slabs * waves * wide, LANES), scratch(slabs, waves * wide, LANES),
            scratch(columns, waves * tall, LANES), scratch(columns, waves * tall, LANES),
            scratch(columns, waves * tall, LANES), scratch(columns, waves * tall, LANES),
            scratch(slabs, waves * wide, LANES), scratch(slabs * waves * wide, LANES),
            narrow((most + 1) * tall, 2 * grid), narrow((most + 1) * tall, 2 * grid),
            scratch(most * tall, 2 * grid),
            *[pltpu.SemaphoreType.DMA((5 + planes // 8,))] * 2,
            *flags(slabs), *flags(columns), *flags(columns), *flags(slabs),
        ],
        compiler_params=pltpu.CompilerParams(
            collective_id=0, has_side_effects=True, vmem_limit_bytes=60 * 1024 * 1024
        ),
        cost_estimate=pl.CostEstimate(
            flops=10**10, bytes_accessed=span_planes * span_rows * grid * 8, transcendentals=0
        ),
        name="solve",
    )(tile, moduli, screening, *(jnp.asarray(t) for t in tables))


def solve_tile(volume, kernel, tables, planes, rows, waves, slabs, columns):
    span_planes, span_rows, grid = volume.shape
    rim_planes = shifted(volume[planes : planes + 3], "gz", 1)
    volume = jnp.concatenate([volume[:3] + rim_planes, volume[3:planes]], 0)
    rim_rows = shifted(volume[:, rows : rows + 3], "gy", 1)
    block = jnp.concatenate([volume[:, :3] + rim_rows, volume[:, 3:rows]], 1)
    potential = potential_field(block, kernel, tables, slabs, columns, waves)
    upper_rows = shifted(potential[:, :3], "gy", -1)
    spare_rows = jnp.zeros((planes, span_rows - rows - 3, grid), jnp.float32)
    widened = jnp.concatenate([potential, upper_rows, spare_rows], 1)
    upper_planes = shifted(widened[:3], "gz", -1)
    spare_planes = jnp.zeros((span_planes - planes - 3, span_rows, grid), jnp.float32)
    return jnp.concatenate([widened, upper_planes, spare_planes], 0)


def body(charge, fractions, cell_base, live_blocks, send_blocks, moduli, screening):
    slabs = lax.axis_size("gz")
    columns = lax.axis_size("gy")
    grid = moduli.shape[1]
    planes = grid // slabs
    rows = grid // columns
    span_planes = round_up(planes + 3 + STEP, 2)
    span_rows = round_up(rows + 3, 8)
    waves = -(-(grid // 2 + 1) // slabs)
    slab = lax.axis_index("gz")
    column = lax.axis_index("gy")
    lane_ids = lax.iota(jnp.int32, columns)
    live = jnp.sum(jnp.where(lane_ids == column, live_blocks[0], 0))
    send = jnp.sum(jnp.where(lane_ids == column, send_blocks[0], 0))
    kept_atoms = (live - send) * BLOCK
    live_atoms = live * BLOCK
    slots = charge.shape[0]
    bits = ((rows - 1).bit_length(), (grid - 1).bit_length())
    slot = lax.iota(jnp.int32, slots)
    key = jnp.where(slot < live_atoms, encode(cell_base, *bits), DEAD)
    key, slot, *values = lax.sort(
        (key, slot, charge, fractions[0], fractions[1], fractions[2]),
        num_keys=1, is_stable=False,
    )
    by_group = key.reshape(slots // GROUP, GROUP)
    alive = by_group < DEAD
    cell_z, cell_y, _ = decode(by_group, *bits)
    bounds = []
    for cell in (cell_z, cell_y):
        high = jnp.max(jnp.where(alive, cell, 0), 1)
        bounds += [jnp.min(jnp.where(alive, cell, high[:, None]), 1), high]
    atoms = [v[None, :] for v in (key, *values)]
    sizes = (span_planes, span_rows, grid)
    count = live_atoms[None]
    tile = spread_atoms(count, bounds, atoms, bits, *sizes).reshape(sizes)
    if fast_sizes(slabs, columns, planes, rows, grid):
        packed_waves = grid // 2 // slabs
        padded = solve_fused(tile, moduli, screening, slabs, columns, planes, rows, packed_waves)
    else:
        tables = wave_tables(grid, slabs, columns, waves)
        kernel = influence(moduli, screening, slab, column, grid, waves, grid // columns)
        padded = solve_tile(tile, kernel, tables, planes, rows, waves, slabs, columns)
    padded = padded.reshape(span_planes * span_rows, grid)
    forces = interpolate_atoms(count, bounds, atoms, padded, bits, *sizes)
    _, *home = lax.sort((slot, *(f[0] for f in forces)), num_keys=1, is_stable=False)
    home = jnp.stack(home)
    margin = SEND_MAX * BLOCK
    room = jnp.concatenate([home, jnp.zeros((3, margin), jnp.float32)], 1)
    lent = lax.dynamic_slice_in_dim(room, kept_atoms, margin, 1)
    moved = shifted(lent, "gy", 1)
    kept = jnp.where(lax.iota(jnp.int32, slots) < kept_atoms, home, 0.0)
    holder = jnp.zeros((3, slots + margin), jnp.float32)
    holder = lax.dynamic_update_slice(holder, moved, (jnp.zeros((), jnp.int32), kept_atoms))
    return kept + holder[:, :slots]


def solution(mesh):
    return jax.shard_map(
        body,
        mesh=mesh,
        in_specs=(
            P(("gz", "gy")),
            P(None, ("gz", "gy")),
            P(None, ("gz", "gy")),
            P("gz", None),
            P("gz", None),
            P(),
            P(),
        ),
        out_specs=P(None, ("gz", "gy")),
        check_vma=False,
    )
```

```python
import functools

import jax
import jax.numpy as jnp
import numpy as np
from jax import lax
from jax.experimental import pallas as pl
from jax.experimental.pallas import tpu as pltpu
from jax.sharding import PartitionSpec as P

BLOCK = 128
SEND_MAX = 36
GROUP = 256
PAIR = 4
LAYER = 2
STEP = 7
WINDOW = 24
CHUNKS = 4
DEAD = 1 << 30

high = lax.Precision.HIGH
coulomb = 2.0


def shifted(x, axis, by):
    peers = lax.axis_size(axis)
    return lax.ppermute(x, axis, [(i, (i + by) % peers) for i in range(peers)])


def round_up(value, step):
    return -(-value // step) * step


def spline_weights(t):
    remain = 1.0 - t
    square = t * t
    cubed = square * t
    weights = [
        remain * remain * remain * (1.0 / 6.0),
        (3.0 * cubed - 6.0 * square + 4.0) * (1.0 / 6.0),
        (-3.0 * cubed + 3.0 * square + 3.0 * t + 1.0) * (1.0 / 6.0),
        cubed * (1.0 / 6.0),
    ]
    slopes = [
        -0.5 * remain * remain,
        1.5 * square - 2.0 * t,
        -1.5 * square + t + 0.5,
        0.5 * square,
    ]
    return weights, slopes


def stencil(base, weights, span):
    offset = lax.broadcasted_iota(jnp.int32, (span, base.shape[1]), 0) - base
    table = jnp.where(offset == 0, weights[0], 0.0)
    for k in range(1, 4):
        table = jnp.where(offset == k, weights[k], table)
    return table


def split(value):
    top = value.astype(jnp.bfloat16)
    rest = (value - top.astype(jnp.float32)).astype(jnp.bfloat16)
    return top, rest


def encode(cells, bits_y, bits_x):
    layer = cells[0] >> LAYER
    flip = (layer & 1) * ((1 << bits_y) - 1)
    inner = cells[0] & ((1 << LAYER) - 1)
    key = (layer << bits_y) | (cells[1] ^ flip)
    return (((key << LAYER) | inner) << bits_x) | cells[2]


def decode(key, bits_y, bits_x):
    inner = (key >> bits_x) & ((1 << LAYER) - 1)
    y = (key >> (bits_x + LAYER)) & ((1 << bits_y) - 1)
    layer = key >> (bits_x + LAYER + bits_y)
    y = y ^ ((layer & 1) * ((1 << bits_y) - 1))
    return (layer << LAYER) | inner, y, key & ((1 << bits_x) - 1)


def wrapped_stencil(places, base, weights, grid):
    top_table = rest_table = jnp.zeros(places.shape, jnp.bfloat16)
    for k in range(4):
        at = base + k
        at = jnp.where(at >= grid, at - grid, at).astype(jnp.float32).astype(jnp.bfloat16)
        hit = places == at
        top, rest = split(weights[k])
        top_table = jnp.where(hit, top, top_table)
        rest_table = jnp.where(hit, rest, rest_table)
    return top_table, rest_table


def fill_places(places):
    places[...] = (
        lax.broadcasted_iota(jnp.int32, places.shape, 0).astype(jnp.float32).astype(jnp.bfloat16)
    )


def over_windows(bounds, group, visit):
    low_z, high_z, low_y, high_y = (bound[group] for bound in bounds)
    start = (low_y // 8) * 8
    steps = (high_z + 3 - low_z) // STEP + 1
    strips = (high_y + 3 - start) // WINDOW + 1
    visit(low_z, start)

    def rest():
        @pl.loop(1, steps * strips)
        def _(at):
            visit(low_z + lax.rem(at, steps) * STEP, start + lax.div(at, steps) * WINDOW)

    return rest


def over_groups(atoms, prepare):
    @pl.loop(0, (atoms + PAIR * GROUP - 1) // (PAIR * GROUP))
    def _(turn):
        later = [prepare(turn * PAIR + i, i) for i in range(PAIR)]
        for rest in later:
            rest()


def spread_kernel(
    rows, grid, bits, count, low_z, high_z, low_y, high_y, key, charge, fz, fy, fx, tile, places, table_z, factor_x,
):
    tile[...] = jnp.zeros_like(tile)
    fill_places(places)
    atoms = count[0]

    def prepare(group, lane):
        at = pl.ds(pl.multiple_of(group * GROUP, GROUP), GROUP)
        place = group * GROUP + lax.broadcasted_iota(jnp.int32, (1, GROUP), 1)
        value = jnp.where(place < atoms, charge[0:1, at], 0.0)
        cell_z, cell_y, cell_x = decode(key[0:1, at], *bits)
        weight_z, _ = spline_weights(fz[0:1, at])
        weight_y, _ = spline_weights(fy[0:1, at])
        weight_x, _ = spline_weights(fx[0:1, at])
        weight_x = [value * w for w in weight_x]
        top, rest = wrapped_stencil(places[...], cell_x, weight_x, grid)
        factor_x[lane, :, :GROUP] = top
        factor_x[lane, :, GROUP:] = rest

        def visit(first, start):
            table_z[lane] = stencil(cell_z - first, weight_z, table_z.shape[1])
            table_y = stencil(cell_y - start, weight_y, WINDOW)
            part = jnp.concatenate([table_z[lane, j : j + 1, :] * table_y for j in range(STEP)], 0)
            top, rest = split(part)
            across = (((1,), (1,)), ((), ()))
            values = lax.dot_general(
                jnp.concatenate([top, rest], 0), factor_x[lane, :, :GROUP], across,
                preferred_element_type=jnp.float32,
            )
            values = values[: STEP * WINDOW] + values[STEP * WINDOW :] + lax.dot_general(
                top, factor_x[lane, :, GROUP:], across, preferred_element_type=jnp.float32
            )
            for j in range(STEP):
                where = pl.ds(pl.multiple_of((first + j) * rows + start, 8), WINDOW)
                tile[where, :] += values[j * WINDOW : (j + 1) * WINDOW, :]

        return over_windows((low_z, high_z, low_y, high_y), group, visit)

    over_groups(atoms, prepare)


def interpolate_kernel(
    rows, grid, bits, count, low_z, high_z, low_y, high_y, key, charge, fz, fy, fx, tile, force_z, force_y, force_x,
    places, factor_x, table_z, rising_z, total,
):
    force_z[...] = jnp.zeros_like(force_z)
    force_y[...] = jnp.zeros_like(force_y)
    force_x[...] = jnp.zeros_like(force_x)
    fill_places(places)
    atoms = count[0]

    def prepare(group, lane):
        at = pl.ds(pl.multiple_of(group * GROUP, GROUP), GROUP)
        place = group * GROUP + lax.broadcasted_iota(jnp.int32, (1, GROUP), 1)
        value = -jnp.where(place < atoms, charge[0:1, at], 0.0)
        cell_z, cell_y, cell_x = decode(key[0:1, at], *bits)
        weight_z, slope_z = spline_weights(fz[0:1, at])
        weight_y, slope_y = spline_weights(fy[0:1, at])
        weight_x, slope_x = spline_weights(fx[0:1, at])
        for half, values in enumerate((weight_x, slope_x)):
            top, rest = wrapped_stencil(places[...], cell_x, values, grid)
            columns = slice(half * GROUP, (half + 1) * GROUP)
            factor_x[lane, :grid, columns] = top
            factor_x[lane, grid:, columns] = rest
        total[lane] = jnp.zeros(total.shape[1:], jnp.float32)

        def visit(first, start):
            span = table_z.shape[1]
            table_z[lane] = stencil(cell_z - first, weight_z, span)
            rising_z[lane] = stencil(cell_z - first, slope_z, span)
            top, rest = split(
                jnp.concatenate(
                    [
                        tile[pl.ds(pl.multiple_of((first + j) * rows + start, 8), WINDOW), :]
                        for j in range(STEP)
                    ],
                    0,
                )
            )
            along = jnp.dot(
                jnp.concatenate([top, rest], 0), factor_x[lane, :grid, :],
                preferred_element_type=jnp.float32,
            )
            along = along[: STEP * WINDOW] + along[STEP * WINDOW :] + jnp.dot(
                top, factor_x[lane, grid:, :], preferred_element_type=jnp.float32
            )
            table_y = stencil(cell_y - start, weight_y, WINDOW)
            rising_y = stencil(cell_y - start, slope_y, WINDOW)
            zs = [table_z[lane, j : j + 1, :] for j in range(STEP)]
            gs = [rising_z[lane, j : j + 1, :] for j in range(STEP)]
            sums = [0.0, 0.0, 0.0]
            for r in range(0, WINDOW, 8):
                local = slice(r, r + 8)
                w = [along[j * WINDOW + r : j * WINDOW + r + 8, :GROUP] for j in range(STEP)]
                s = [along[j * WINDOW + r : j * WINDOW + r + 8, GROUP:] for j in range(STEP)]
                sums[0] += table_y[local] * sum(gs[j] * w[j] for j in range(STEP))
                sums[1] += rising_y[local] * sum(zs[j] * w[j] for j in range(STEP))
                sums[2] += table_y[local] * sum(zs[j] * s[j] for j in range(STEP))
            for i in range(3):
                total[lane, 8 * i : 8 * i + 8, :] += sums[i]

        rest_of = over_windows((low_z, high_z, low_y, high_y), group, visit)

        def finish():
            rest_of()
            for i, force in enumerate((force_z, force_y, force_x)):
                part = total[lane, 8 * i : 8 * i + 8, :]
                force[0:1, at] = value * jnp.sum(part, 0, keepdims=True)

        return finish

    over_groups(atoms, prepare)


def vmem():
    return pl.BlockSpec(memory_space=pltpu.VMEM)


def smem():
    return pl.BlockSpec(memory_space=pltpu.SMEM)


def spread_atoms(count, bounds, atoms, bits, planes, rows, grid):
    slots = atoms[0].shape[1]
    return pl.pallas_call(
        functools.partial(spread_kernel, rows, grid, bits),
        out_shape=jax.ShapeDtypeStruct((planes * rows, grid), jnp.float32),
        in_specs=[smem()] * 5 + [vmem()] * 5,
        out_specs=vmem(),
        scratch_shapes=[
            pltpu.VMEM((grid, GROUP), jnp.bfloat16),
            pltpu.VMEM((PAIR, 8, GROUP), jnp.float32),
            pltpu.VMEM((PAIR, grid, 2 * GROUP), jnp.bfloat16),
        ],
        cost_estimate=pl.CostEstimate(
            flops=STEP * rows * grid * slots * 6,
            bytes_accessed=planes * rows * grid * 4,
            transcendentals=0,
        ),
        compiler_params=pltpu.CompilerParams(

        ),
        name="spread",
    )(count, *bounds, *atoms)


def interpolate_atoms(count, bounds, atoms, tile, bits, planes, rows, grid):
    slots = atoms[0].shape[1]
    return pl.pallas_call(
        functools.partial(interpolate_kernel, rows, grid, bits),
        out_shape=[jax.ShapeDtypeStruct((1, slots), jnp.float32)] * 3,
        in_specs=[smem()] * 5 + [vmem()] * 6,
        out_specs=[vmem()] * 3,
        scratch_shapes=[
            pltpu.VMEM((grid, GROUP), jnp.bfloat16),
            pltpu.VMEM((PAIR, 2 * grid, 2 * GROUP), jnp.bfloat16),
            pltpu.VMEM((PAIR, 8, GROUP), jnp.float32),
            pltpu.VMEM((PAIR, 8, GROUP), jnp.float32),
            pltpu.VMEM((PAIR, 24, GROUP), jnp.float32),
        ],
        cost_estimate=pl.CostEstimate(
            flops=STEP * rows * grid * slots * 12,
            bytes_accessed=planes * rows * grid * 4,
            transcendentals=0,
        ),
        name="interpolate",
    )(count, *bounds, *atoms, tile)


def turns(grid, wave, place, quarter):
    whole = np.mod(wave * place + (grid // 4) * quarter, grid)
    return np.cos(2.0 * np.pi * whole / grid).astype(np.float32)


def wave_tables(grid, slabs, columns, waves):
    kx = np.arange(slabs * waves).reshape(slabs, 1, waves)
    part = np.arange(2)
    x = np.arange(grid)
    table_x = turns(grid, kx[None], x[:, None, None, None], part[None, None, :, None])
    kz = np.arange(grid).reshape(columns, 1, grid // columns, 1, 1)
    table_z = turns(
        grid, kz, x[None, None, None, :, None],
        part[None, :, None, None, None] - part[None, None, None, None, :],
    ).reshape(2 * grid, 2 * grid)
    y = np.arange(grid).reshape(columns, 1, grid // columns, 1, 1)
    table_y = turns(
        grid, x[None, None, None, None, :], y,
        part[None, None, None, :, None] - part[None, :, None, None, None],
    )
    return table_x, table_z, table_y


def signed_wave(waves, grid):
    return jnp.where(waves < grid // 2, waves, waves - grid)


def influence(moduli, screening, slab, column, grid, count_kx, count_kz):
    kx = slab * count_kx + lax.iota(jnp.int32, count_kx)
    kz = column * count_kz + lax.iota(jnp.int32, count_kz)
    ky = lax.iota(jnp.int32, grid)
    half = grid // 2
    share = jnp.where((kx == 0) | (kx == half), 1.0, 2.0)
    share = jnp.where(kx <= half, share, 0.0) * (0.5 * coulomb / grid**3)
    nx, nz, ny = (signed_wave(k, grid) for k in (kx, kz, ky))
    radius = (nz * nz)[:, None, None] + (nx * nx)[None, :, None] + (ny * ny)[None, None, :]
    squared = radius.astype(jnp.float32) / float(grid * grid)
    mirrored = jnp.roll(moduli[:, ::-1], 1, 1)
    spare = jnp.zeros((count_kx * lax.axis_size("gz"),), jnp.float32)

    def product(table):
        mx = lax.dynamic_slice_in_dim(
            jnp.concatenate([table[2], spare]), slab * count_kx, count_kx, 0
        )
        mz = lax.dynamic_slice_in_dim(table[0], column * count_kz, count_kz, 0)
        return mz[:, None, None] * (share * mx)[None, :, None] * table[1][None, None, :]

    both = product(moduli) + product(mirrored)
    safe = jnp.where(radius > 0, squared, 1.0)
    return jnp.where(radius > 0, both * jnp.exp(-screening[0] * squared) / safe, 0.0)


def exchange(x, axis):
    return lax.all_to_all(x, axis, split_axis=0, concat_axis=0, tiled=True)


def contract(form, *operands):
    return jnp.einsum(form, *operands, precision=high, preferred_element_type=jnp.float32)


def potential_field(block, kernel, tables, slabs, columns, waves):
    table_x, table_z, table_y = tables
    planes, rows, grid = block.shape
    lanes = waves * rows
    spectrum = contract("zyx,xpck->pzcky", block, table_x)
    spectrum = exchange(spectrum.reshape(slabs * planes * 2, lanes), "gz")
    spectrum = contract("mn,nl->ml", table_z, spectrum)
    spectrum = exchange(spectrum, "gy").reshape(columns, 2, grid // columns, waves, rows)
    spectrum = contract("pczky,pcydw->zkdw", spectrum, table_y)
    spectrum = spectrum * kernel[:, :, None, :]
    spectrum = contract("zkdw,pcydw->pczky", spectrum, table_y)
    spectrum = exchange(spectrum.reshape(2 * grid, lanes), "gy")
    spectrum = contract("mn,ml->nl", table_z, spectrum)
    spectrum = exchange(spectrum, "gz").reshape(slabs, planes, 2, waves, rows)
    return contract("pzcky,xpck->zyx", spectrum, table_x)


LANES = 128
MESH = pl.DeviceIdType.MESH


def fast_sizes(slabs, columns, planes, rows, grid):
    return (
        2 * rows == LANES
        and grid == 2 * LANES
        and columns * rows == grid
        and slabs * planes == grid
        and planes % 8 == 0
        and LANES % (2 * columns) == 0
        and LANES % slabs == 0
        and slabs >= 3
        and columns >= 3
    )


def kept_waves(half, columns):
    pairs = [k for n in range(1, half // 2) for k in (n, half - n)]
    return np.array([0, half // 2] + pairs).reshape(columns, half // columns)


def partners(half, columns):
    share = half // columns
    moves = np.zeros((columns, 2 * share, 2 * share), np.float32)
    for c, waves in enumerate(kept_waves(half, columns)):
        place = {int(k): j for j, k in enumerate(waves)}
        for h in range(2):
            for k, j in place.items():
                other = (2 * half - h * half - k) % (2 * half)
                moves[c, h * share + j, other // half * share + place[other % half]] = 1.0
    return moves.astype(jnp.bfloat16)


def fill_green(green, moduli, screening, slab, column, waves, columns):
    grid = moduli.shape[1]
    half = grid // 2
    share = half // columns
    tall = 2 * share

    def signed(k):
        return jnp.where(k < half, k, k - grid)

    def opposite(k):
        return jnp.where(k == 0, 0, grid - k)

    def pick(lanes, at, values):
        return jnp.sum(jnp.where(lanes == at, values, 0.0), 1, keepdims=True)

    down = lax.broadcasted_iota(jnp.int32, (grid, grid), 0)
    over = lax.broadcasted_iota(jnp.int32, (grid, grid), 1)
    turned = pick(over, opposite(down), moduli[1:2, :])
    factor_y = moduli[1:2, :]
    mirror_y = jnp.sum(jnp.where(down == over, turned, 0.0), 0, keepdims=True)
    lanes = over[:tall]
    row = down[:tall]
    upper = jnp.where(row >= share, 1, 0)
    place = column * share + row - upper * share
    kept = jnp.where((place & 1) == 0, place >> 1, half - (place >> 1))
    kz = upper * half + jnp.where(place == 1, half // 2, kept)
    factor_z = pick(lanes, kz, moduli[0:1, :])
    mirror_z = pick(lanes, opposite(kz), moduli[0:1, :])
    flat = signed(kz) * signed(kz) + signed(lanes) * signed(lanes)

    def values(kx):
        share_x = jnp.where((kx == 0) | (kx == half), 1.0, 2.0) * (0.5 * coulomb / grid**3)
        factor_x = share_x * pick(over[:1], kx, moduli[2:3, :])
        mirror_x = share_x * pick(over[:1], opposite(kx), moduli[2:3, :])
        both = factor_x * factor_z * factor_y + mirror_x * mirror_z * mirror_y
        radius = flat + signed(kx) * signed(kx)
        squared = radius.astype(jnp.float32) * (1.0 / (grid * grid))
        safe = jnp.where(radius > 0, squared, 1.0)
        return jnp.where(radius > 0, both * jnp.exp(-screening[0] * squared) / safe, 0.0)

    plain = values(slab * waves)
    ends = values(half)
    green[:tall, :] = jnp.where(slab == 0, 0.5 * (plain + ends), plain)
    green[waves * tall :, :] = jnp.where(slab == 0, 0.5 * (plain - ends), 0.0)

    @pl.loop(1, waves)
    def _(w):
        green[pl.ds(pl.multiple_of(w * tall, tall), tall), :] = values(slab * waves + w)


def halves(table):
    table = np.ascontiguousarray(table, dtype=np.float32)
    top = table.astype(jnp.bfloat16)
    rest = (table - top.astype(np.float32)).astype(jnp.bfloat16)
    return top, rest


def solve_tables(grid, slabs, columns, waves, planes):
    half = grid // 2
    pairs = planes // 2
    share = half // columns
    x = np.arange(grid)
    part = np.arange(2)
    kx = np.repeat(np.arange(slabs * waves), 2)
    px = np.tile(part, slabs * waves)
    table_x = turns(grid, kx[:, None], x[None, :], px[:, None])
    table_x[1] = np.where(x % 2, -1.0, 1.0)
    forward_x = np.concatenate(halves(table_x))
    inverse_x = np.concatenate(halves(table_x.T))
    kept = kept_waves(half, columns)
    kz = np.broadcast_to(kept[:, None, :], (columns, 2, share)).reshape(-1)
    pk = np.broadcast_to(part.reshape(1, 2, 1), (columns, 2, share)).reshape(-1)
    zh = np.broadcast_to(np.arange(half).reshape(slabs, 1, pairs), (slabs, 2, pairs)).reshape(-1)
    pz = np.broadcast_to(part.reshape(1, 2, 1), (slabs, 2, pairs)).reshape(-1)
    table_z = turns(half, kz[:, None], zh[None, :], pk[:, None] - pz[None, :])
    forward_z = np.stack(halves(table_z))
    inverse_z = np.stack(halves(table_z.T))
    ky = np.tile(np.arange(grid), 2)
    pf = np.repeat(part, grid)
    table_y = turns(grid, ky[:, None], ky[None, :], pf[None, :] - pf[:, None])
    forward_y = np.stack(halves(table_y))
    angle = 2.0 * np.pi * kept.reshape(-1, 1) / grid
    upper = np.arange(LANES)[None, :] >= LANES // 2
    twist = np.stack(
        [np.where(upper, np.cos(angle), 1.0), np.where(upper, np.sin(angle), 0.0)]
    ).astype(np.float32)
    return forward_x, inverse_x, forward_z, inverse_z, forward_y, twist, partners(half, columns)


def chunks_of(waves, count):
    edges = [waves * i // count for i in range(count + 1)]
    return [(a, b - a) for a, b in zip(edges, edges[1:]) if b > a]


def solve_kernel(
    slabs, columns, waves, planes, rows, grid, chunks,
    tile, moduli, screening, table_fx, *rest_of,
):
    late, out, green = rest_of[:6], rest_of[6], rest_of[7]
    tables, table_sems = rest_of[8:14], rest_of[14]
    (
        rim_z, rim_y, rim_c,
        x_out, z_in, z_out, y_in, y_out, z_back, z_send, x_in, y_top, y_rest, y_right,
        rim_send, rim_recv, gz_send, gz_recv, gy_send, gy_recv, by_send, by_recv, bz_send, bz_recv,
    ) = rest_of[15:]
    table_ix, table_fz, table_iz, table_y, twist, moves = tables
    half = grid // 2
    pairs = planes // 2
    wide = 2 * pairs
    share = half // columns
    tall = 2 * share
    bins = 2 * slabs * waves
    slab = lax.axis_index("gz")
    column = lax.axis_index("gy")

    def around(step):
        return lax.rem(slab + step + slabs, slabs)

    def beside(step):
        return lax.rem(column + step + columns, columns)

    barrier = pltpu.get_barrier_semaphore()
    for step in range(1, slabs):
        pl.semaphore_signal(barrier, inc=1, device_id=(around(step), column), device_id_type=MESH)
    for step in range(1, columns):
        pl.semaphore_signal(barrier, inc=1, device_id=(slab, beside(step)), device_id_type=MESH)
    for step in (1, -1):
        pl.semaphore_signal(
            barrier, inc=1, device_id=(around(step), beside(step)), device_id_type=MESH
        )
    pl.semaphore_wait(barrier, slabs + columns)

    def remote(source, target, sends, recvs, at, to):
        return pltpu.make_async_remote_copy(
            src_ref=source, dst_ref=target, send_sem=sends.at[at], recv_sem=recvs.at[at],
            device_id=to, device_id_type=MESH,
        )

    main, edge = pl.ds(0, rows), pl.ds(rows, 8)
    body_z, over_z = pl.ds(0, planes), pl.ds(planes, 3)
    rims = [
        remote(tile.at[over_z, main], rim_z, rim_send, rim_recv, 0, (around(1), column)),
        remote(tile.at[body_z, edge], rim_y, rim_send, rim_recv, 1, (slab, beside(1))),
        remote(tile.at[over_z, edge], rim_c, rim_send, rim_recv, 2, (around(1), beside(1))),
    ]
    for copy in rims:
        copy.start()
    fetches = [
        pltpu.make_async_copy(source, target, table_sems.at[i])
        for i, (source, target) in enumerate(zip(late, tables))
    ]
    for fetch in fetches:
        fetch.start()

    out[planes + 3 :] = jnp.zeros_like(out[planes + 3 :])
    across = (((1,), (1,)), ((), ()))

    def product(left, right, form=(((1,), (0,)), ((), ()))):
        return lax.dot_general(left, right, form, preferred_element_type=jnp.float32)

    def along_x(at, rim):
        value = tile[pl.ds(at * 4, 4), :rows, :]
        head = value[:, :8] + rim_y[pl.ds(at * 4, 4)]
        value = jnp.concatenate([head, value[:, 8:]], 1)
        if rim is not None:
            value = value + jnp.concatenate([rim, jnp.zeros((1, rows, grid), jnp.float32)], 0)
        top, rest = split(value.reshape(4 * rows, grid))
        both = product(table_fx[...], top, across)
        values = both[:bins] + both[bins:] + product(table_fx[:bins, :], rest, across)
        for side in range(2):
            where = pl.ds(2 * at + side, bins, stride=pairs)
            x_out[where, :] = values[:, side * LANES : (side + 1) * LANES]

    rims[1].wait()

    @pl.loop(0, (planes // 4 - 2) // 2)
    def _(turn_at):
        along_x(2 * turn_at + 1, None)
        along_x(2 * turn_at + 2, None)

    rims[0].wait()
    rims[2].wait()
    rim_z[:, :8, :] += rim_c[...]
    along_x(planes // 4 - 1, None)
    along_x(0, rim_z[...])

    def gz_copy(q, step):
        w, n = chunks[q]
        source = x_out.at[pl.ds((around(step) * waves + w) * wide, n * wide)]
        target = z_in.at[slab, pl.ds(w * wide, n * wide)]
        return remote(source, target, gz_send, gz_recv, (q, step), (around(step), column))

    def gy_copy(q, step):
        w, n = chunks[q]
        where = pl.ds(w * tall, n * tall)
        source, target = z_out.at[beside(step), where], y_in.at[column, where]
        return remote(source, target, gy_send, gy_recv, (q, step), (slab, beside(step)))

    def by_copy(q, step):
        w, n = chunks[q]
        where = pl.ds(w * tall, n * tall)
        source, target = y_out.at[beside(step), where], z_back.at[column, where]
        return remote(source, target, by_send, by_recv, (q, step), (slab, beside(step)))

    def bz_copy(q, step):
        w, n = chunks[q]
        source = z_send.at[around(step), pl.ds(w * wide, n * wide)]
        target = x_in.at[pl.ds((slab * waves + w) * wide, n * wide)]
        return remote(source, target, bz_send, bz_recv, (q, step), (around(step), column))

    for q in range(len(chunks)):
        for step in range(1, slabs):
            gz_copy(q, step).start()
    z_in[slab] = x_out[pl.ds(pl.multiple_of(slab * waves * wide, wide), waves * wide), :]

    for fetch in fetches:
        fetch.wait()
    fill_green(green, moduli, screening, slab, column, waves, columns)
    left = lax.broadcasted_iota(jnp.int32, (half, LANES), 1) < LANES // 2
    side = left[:share]

    def turn(value):
        return pltpu.roll(value, LANES // 2, 1)

    def along_z(table, value):
        top, rest = split(value)
        both = product(table[0], jnp.concatenate([top, rest], 1))
        return both[:, :LANES] + both[:, LANES:] + product(table[1], top)

    def to_z(q):
        for step in range(1, slabs):
            gz_copy(q, step).wait_recv()
        first, count = chunks[q]

        @pl.loop(first, first + count)
        def _(w):
            value = z_in[:, pl.ds(pl.multiple_of(w * wide, wide), wide), :].reshape(grid, LANES)
            value = along_z(table_fz, value)
            value = value.reshape(columns, 2, share, LANES)
            re = value[:, 0].reshape(half, LANES)
            im = value[:, 1].reshape(half, LANES)
            re, im = re * twist[0] + im * twist[1], im * twist[0] - re * twist[1]
            for p, v in enumerate((re, im)):
                v = jnp.where(left, v + turn(v), turn(v) - v)
                where = pl.ds(pl.multiple_of(w * tall + p * share, share), share)
                z_out[:, where, :] = v.reshape(columns, share, LANES)

        for step in range(1, columns):
            gy_copy(q, step).start()
        where = pl.ds(first * tall, count * tall)
        y_in[column, where, :] = z_out[column, where, :]

    def to_y(q):
        for step in range(1, columns):
            gy_copy(q, step).wait_recv()
        first, count = chunks[q]

        @pl.loop(0, count)
        def _(w):
            for p in range(2):
                where = pl.ds(pl.multiple_of((first + w) * tall + p * share, share), share)
                for c in range(0, columns, 2):
                    a, b = y_in[c, where, :], y_in[c + 1, where, :]
                    pair = (jnp.where(side, a, turn(b)), jnp.where(side, turn(a), b))
                    for h in range(2):
                        to = pl.ds(pl.multiple_of(w * tall + h * share, share), share)
                        at = (p * columns + c) * rows
                        top, rest = split(pair[h])
                        y_top[to, at : at + LANES] = top
                        y_rest[to, at : at + LANES] = rest

        main_rows = size = count * tall
        if first == 0:
            size += tall
            for target in (y_top, y_rest):
                value = product(moves[column], target[:tall, :])
                value = jnp.concatenate([value[:, :grid], -value[:, grid:]], 1)
                target[main_rows:size, :] = value.astype(jnp.bfloat16)
        top = y_top[:size, :]
        both = product(jnp.concatenate([top, y_rest[:size, :]], 0), table_y[0])
        value = both[:size] + both[size:] + product(top, table_y[1])
        factor = green[first * tall : (first + count) * tall, :]
        if first == 0:
            factor = jnp.concatenate([factor, green[waves * tall :, :]], 0)
        value = jnp.concatenate([value[:, :grid] * factor, value[:, grid:] * factor], 1)
        if first == 0:
            value = jnp.concatenate([value[:tall] + value[main_rows:], value[tall:main_rows]], 0)
        size = main_rows
        top, rest = split(value)
        both = product(jnp.concatenate([top, rest], 0), table_y[0], across)
        y_right[:size, :] = both[:size] + both[size:] + product(top, table_y[1], across)

        @pl.loop(0, count)
        def _(w):
            for p in range(2):
                where = pl.ds(pl.multiple_of((first + w) * tall + p * share, share), share)
                for c in range(0, columns, 2):
                    at = (p * columns + c) * rows
                    a, b = (
                        y_right[
                            pl.ds(pl.multiple_of(w * tall + h * share, share), share),
                            at : at + LANES,
                        ]
                        for h in range(2)
                    )
                    y_out[c, where, :] = jnp.where(side, a, turn(b))
                    y_out[c + 1, where, :] = jnp.where(side, turn(a), b)

        for step in range(1, columns):
            by_copy(q, step).start()
        where = pl.ds(first * tall, count * tall)
        z_back[column, where, :] = y_out[column, where, :]

    def from_z(q):
        for step in range(1, columns):
            by_copy(q, step).wait_recv()
        first, count = chunks[q]

        @pl.loop(first, first + count)
        def _(w):
            value = z_back[:, pl.ds(pl.multiple_of(w * tall, tall), tall), :]
            re = value[:, :share].reshape(half, LANES)
            im = value[:, share:].reshape(half, LANES)
            re, im = (jnp.where(left, v + turn(v), turn(v) - v) for v in (re, im))
            re, im = re * twist[0] - im * twist[1], im * twist[0] + re * twist[1]
            re, im = (v.reshape(columns, share, LANES) for v in (re, im))
            value = jnp.concatenate(
                [v[c] for c in range(columns) for v in (re, im)], 0
            )
            value = along_z(table_iz, value)
            where = pl.ds(pl.multiple_of(w * wide, wide), wide)
            z_send[:, where, :] = value.reshape(slabs, wide, LANES)

        for step in range(1, slabs):
            bz_copy(q, step).start()
        where = pl.ds(pl.multiple_of((slab * waves + first) * wide, wide), count * wide)
        x_in[where, :] = z_send[slab, pl.ds(first * wide, count * wide), :]

    stages = (to_z, to_y, from_z)
    for turn_at in range(len(chunks) + len(stages) - 1):
        for at, stage in enumerate(stages):
            if 0 <= turn_at - at < len(chunks):
                stage(turn_at - at)
    for q in range(len(chunks)):
        for step in range(1, slabs):
            bz_copy(q, step).wait_recv()

    def back_x(at):
        value = jnp.concatenate(
            [x_in[pl.ds(2 * at + s, bins, stride=pairs), :] for s in range(2)], 1
        )
        top, rest = split(value)
        both = product(table_ix[...], top)
        value = both[:grid] + both[grid:] + product(table_ix[:grid, :], rest)
        out[pl.ds(at * 4, 4), :rows, :] = value.T.reshape(4, rows, grid)

    def rim_back(at):
        planes_of = pl.ds(8 * at, 8)
        return remote(
            out.at[planes_of, pl.ds(0, 8)], out.at[planes_of, edge],
            rim_send, rim_recv, 5 + at, (slab, beside(-1)),
        )

    rims_back = [rim_back(at) for at in range(planes // 8)] + [
        remote(
            out.at[pl.ds(0, 3), main], out.at[over_z, main],
            rim_send, rim_recv, 3, (around(-1), column),
        ),
        remote(
            out.at[pl.ds(0, 3), pl.ds(0, 8)], out.at[over_z, edge],
            rim_send, rim_recv, 4, (around(-1), beside(-1)),
        ),
    ]
    for at in range(planes // 8):
        back_x(2 * at)
        back_x(2 * at + 1)
        if at == 0:
            for copy in rims_back[-2:]:
                copy.start()
        else:
            rims_back[at - 1].start()
    rims_back[planes // 8 - 1].start()
    for q in range(len(chunks)):
        for copy, steps in (
            (gz_copy, slabs), (gy_copy, columns), (by_copy, columns), (bz_copy, slabs)
        ):
            for step in range(1, steps):
                copy(q, step).wait_send()
    for copy in rims_back:
        copy.wait()


def solve_fused(tile, moduli, screening, slabs, columns, planes, rows, waves):
    span_planes, span_rows, grid = tile.shape
    tables = solve_tables(grid, slabs, columns, waves, planes)
    chunks = chunks_of(waves, CHUNKS)
    most = max(n for _, n in chunks)
    wide, tall = planes, 2 * (grid // 2 // columns)

    def scratch(*shape):
        return pltpu.VMEM(shape, jnp.float32)

    def narrow(*shape):
        return pltpu.VMEM(shape, jnp.bfloat16)

    def flags(count):
        return [pltpu.SemaphoreType.DMA((len(chunks), count))] * 2

    return pl.pallas_call(
        functools.partial(
            solve_kernel, slabs, columns, waves, planes, rows, grid, chunks
        ),
        out_shape=jax.ShapeDtypeStruct(tile.shape, jnp.float32),
        in_specs=[vmem()] * 2 + [smem(), vmem()]
        + [pl.BlockSpec(memory_space=pl.ANY)] * 6,
        out_specs=vmem(),
        scratch_shapes=[
            scratch((waves + 1) * tall, grid),
            *[pltpu.VMEM(t.shape, t.dtype) for t in tables[1:]],
            pltpu.SemaphoreType.DMA((6,)),
            scratch(3, rows, grid), scratch(planes, 8, grid), scratch(3, 8, grid),
            scratch(slabs * waves * wide, LANES), scratch(slabs, waves * wide, LANES),
            scratch(columns, waves * tall, LANES), scratch(columns, waves * tall, LANES),
            scratch(columns, waves * tall, LANES), scratch(columns, waves * tall, LANES),
            scratch(slabs, waves * wide, LANES), scratch(slabs * waves * wide, LANES),
            narrow((most + 1) * tall, 2 * grid), narrow((most + 1) * tall, 2 * grid),
            scratch(most * tall, 2 * grid),
            *[pltpu.SemaphoreType.DMA((5 + planes // 8,))] * 2,
            *flags(slabs), *flags(columns), *flags(columns), *flags(slabs),
        ],
        compiler_params=pltpu.CompilerParams(
            collective_id=0, has_side_effects=True, vmem_limit_bytes=60 * 1024 * 1024
        ),
        cost_estimate=pl.CostEstimate(
            flops=10**10, bytes_accessed=span_planes * span_rows * grid * 8, transcendentals=0
        ),
        name="solve",
    )(tile, moduli, screening, *(jnp.asarray(t) for t in tables))


def solve_tile(volume, kernel, tables, planes, rows, waves, slabs, columns):
    span_planes, span_rows, grid = volume.shape
    rim_planes = shifted(volume[planes : planes + 3], "gz", 1)
    volume = jnp.concatenate([volume[:3] + rim_planes, volume[3:planes]], 0)
    rim_rows = shifted(volume[:, rows : rows + 3], "gy", 1)
    block = jnp.concatenate([volume[:, :3] + rim_rows, volume[:, 3:rows]], 1)
    potential = potential_field(block, kernel, tables, slabs, columns, waves)
    upper_rows = shifted(potential[:, :3], "gy", -1)
    spare_rows = jnp.zeros((planes, span_rows - rows - 3, grid), jnp.float32)
    widened = jnp.concatenate([potential, upper_rows, spare_rows], 1)
    upper_planes = shifted(widened[:3], "gz", -1)
    spare_planes = jnp.zeros((span_planes - planes - 3, span_rows, grid), jnp.float32)
    return jnp.concatenate([widened, upper_planes, spare_planes], 0)


def body(charge, fractions, cell_base, live_blocks, send_blocks, moduli, screening):
    slabs = lax.axis_size("gz")
    columns = lax.axis_size("gy")
    grid = moduli.shape[1]
    planes = grid // slabs
    rows = grid // columns
    span_planes = round_up(planes + 3 + STEP, 2)
    span_rows = round_up(rows + 3, 8)
    waves = -(-(grid // 2 + 1) // slabs)
    slab = lax.axis_index("gz")
    column = lax.axis_index("gy")
    lane_ids = lax.iota(jnp.int32, columns)
    live = jnp.sum(jnp.where(lane_ids == column, live_blocks[0], 0))
    send = jnp.sum(jnp.where(lane_ids == column, send_blocks[0], 0))
    kept_atoms = (live - send) * BLOCK
    live_atoms = live * BLOCK
    slots = charge.shape[0]
    bits = ((rows - 1).bit_length(), (grid - 1).bit_length())
    slot = lax.iota(jnp.int32, slots)
    key = jnp.where(slot < live_atoms, encode(cell_base, *bits), DEAD)
    key, slot, *values = lax.sort(
        (key, slot, charge, fractions[0], fractions[1], fractions[2]),
        num_keys=1, is_stable=False,
    )
    by_group = key.reshape(slots // GROUP, GROUP)
    alive = by_group < DEAD
    cell_z, cell_y, _ = decode(by_group, *bits)
    bounds = []
    for cell in (cell_z, cell_y):
        high = jnp.max(jnp.where(alive, cell, 0), 1)
        bounds += [jnp.min(jnp.where(alive, cell, high[:, None]), 1), high]
    atoms = [v[None, :] for v in (key, *values)]
    sizes = (span_planes, span_rows, grid)
    count = live_atoms[None]
    tile = spread_atoms(count, bounds, atoms, bits, *sizes).reshape(sizes)
    if fast_sizes(slabs, columns, planes, rows, grid):
        packed_waves = grid // 2 // slabs
        padded = solve_fused(tile, moduli, screening, slabs, columns, planes, rows, packed_waves)
    else:
        tables = wave_tables(grid, slabs, columns, waves)
        kernel = influence(moduli, screening, slab, column, grid, waves, grid // columns)
        padded = solve_tile(tile, kernel, tables, planes, rows, waves, slabs, columns)
    padded = padded.reshape(span_planes * span_rows, grid)
    forces = interpolate_atoms(count, bounds, atoms, padded, bits, *sizes)
    _, *home = lax.sort((slot, *(f[0] for f in forces)), num_keys=1, is_stable=False)
    home = jnp.stack(home)
    margin = SEND_MAX * BLOCK
    room = jnp.concatenate([home, jnp.zeros((3, margin), jnp.float32)], 1)
    lent = lax.dynamic_slice_in_dim(room, kept_atoms, margin, 1)
    moved = shifted(lent, "gy", 1)
    kept = jnp.where(lax.iota(jnp.int32, slots) < kept_atoms, home, 0.0)
    holder = jnp.zeros((3, slots + margin), jnp.float32)
    holder = lax.dynamic_update_slice(holder, moved, (jnp.zeros((), jnp.int32), kept_atoms))
    return kept + holder[:, :slots]


def solution(mesh):
    return jax.shard_map(
        body,
        mesh=mesh,
        in_specs=(
            P(("gz", "gy")),
            P(None, ("gz", "gy")),
            P(None, ("gz", "gy")),
            P("gz", None),
            P("gz", None),
            P(),
            P(),
        ),
        out_specs=P(None, ("gz", "gy")),
        check_vma=False,
    )
```

```python
import functools

import jax
import jax.numpy as jnp
import numpy as np
from jax import lax
from jax.experimental import pallas as pl
from jax.experimental.pallas import tpu as pltpu
from jax.sharding import PartitionSpec as P

BLOCK = 128
SEND_MAX = 36
GROUP = 256
PAIR = 4
LAYER = 2
STEP = 7
WINDOW = 24
CHUNKS = 4
DEAD = 1 << 30

high = lax.Precision.HIGH
coulomb = 2.0


def shifted(x, axis, by):
    peers = lax.axis_size(axis)
    return lax.ppermute(x, axis, [(i, (i + by) % peers) for i in range(peers)])


def round_up(value, step):
    return -(-value // step) * step


def spline_weights(t):
    remain = 1.0 - t
    square = t * t
    cubed = square * t
    weights = [
        remain * remain * remain * (1.0 / 6.0),
        (3.0 * cubed - 6.0 * square + 4.0) * (1.0 / 6.0),
        (-3.0 * cubed + 3.0 * square + 3.0 * t + 1.0) * (1.0 / 6.0),
        cubed * (1.0 / 6.0),
    ]
    slopes = [
        -0.5 * remain * remain,
        1.5 * square - 2.0 * t,
        -1.5 * square + t + 0.5,
        0.5 * square,
    ]
    return weights, slopes


def stencil(base, weights, span):
    offset = lax.broadcasted_iota(jnp.int32, (span, base.shape[1]), 0) - base
    table = jnp.where(offset == 0, weights[0], 0.0)
    for k in range(1, 4):
        table = jnp.where(offset == k, weights[k], table)
    return table


def split(value):
    top = value.astype(jnp.bfloat16)
    rest = (value - top.astype(jnp.float32)).astype(jnp.bfloat16)
    return top, rest


def encode(cells, bits_y, bits_x):
    layer = cells[0] >> LAYER
    flip = (layer & 1) * ((1 << bits_y) - 1)
    inner = cells[0] & ((1 << LAYER) - 1)
    key = (layer << bits_y) | (cells[1] ^ flip)
    return (((key << LAYER) | inner) << bits_x) | cells[2]


def decode(key, bits_y, bits_x):
    inner = (key >> bits_x) & ((1 << LAYER) - 1)
    y = (key >> (bits_x + LAYER)) & ((1 << bits_y) - 1)
    layer = key >> (bits_x + LAYER + bits_y)
    y = y ^ ((layer & 1) * ((1 << bits_y) - 1))
    return (layer << LAYER) | inner, y, key & ((1 << bits_x) - 1)


def wrapped_stencil(places, base, weights, grid):
    top_table = rest_table = jnp.zeros(places.shape, jnp.bfloat16)
    for k in range(4):
        at = base + k
        at = jnp.where(at >= grid, at - grid, at).astype(jnp.float32).astype(jnp.bfloat16)
        hit = places == at
        top, rest = split(weights[k])
        top_table = jnp.where(hit, top, top_table)
        rest_table = jnp.where(hit, rest, rest_table)
    return top_table, rest_table


def fill_places(places):
    places[...] = (
        lax.broadcasted_iota(jnp.int32, places.shape, 0).astype(jnp.float32).astype(jnp.bfloat16)
    )


def over_windows(bounds, group, visit):
    low_z, high_z, low_y, high_y = (bound[group] for bound in bounds)
    start = (low_y // 8) * 8
    steps = (high_z + 3 - low_z) // STEP + 1
    strips = (high_y + 3 - start) // WINDOW + 1
    visit(low_z, start)

    def rest():
        @pl.loop(1, steps * strips)
        def _(at):
            visit(low_z + lax.rem(at, steps) * STEP, start + lax.div(at, steps) * WINDOW)

    return rest


def over_groups(atoms, prepare):
    @pl.loop(0, (atoms + PAIR * GROUP - 1) // (PAIR * GROUP))
    def _(turn):
        later = [prepare(turn * PAIR + i, i) for i in range(PAIR)]
        for rest in later:
            rest()


def spread_kernel(
    rows, grid, bits, count, low_z, high_z, low_y, high_y, key, charge, fz, fy, fx, tile, places, table_z, factor_x,
):
    tile[...] = jnp.zeros_like(tile)
    fill_places(places)
    atoms = count[0]

    def prepare(group, lane):
        at = pl.ds(pl.multiple_of(group * GROUP, GROUP), GROUP)
        place = group * GROUP + lax.broadcasted_iota(jnp.int32, (1, GROUP), 1)
        value = jnp.where(place < atoms, charge[0:1, at], 0.0)
        cell_z, cell_y, cell_x = decode(key[0:1, at], *bits)
        weight_z, _ = spline_weights(fz[0:1, at])
        weight_y, _ = spline_weights(fy[0:1, at])
        weight_x, _ = spline_weights(fx[0:1, at])
        weight_x = [value * w for w in weight_x]
        top, rest = wrapped_stencil(places[...], cell_x, weight_x, grid)
        factor_x[lane, :, :GROUP] = top
        factor_x[lane, :, GROUP:] = rest

        def visit(first, start):
            table_z[lane] = stencil(cell_z - first, weight_z, table_z.shape[1])
            table_y = stencil(cell_y - start, weight_y, WINDOW)
            part = jnp.concatenate([table_z[lane, j : j + 1, :] * table_y for j in range(STEP)], 0)
            top, rest = split(part)
            across = (((1,), (1,)), ((), ()))
            values = lax.dot_general(
                jnp.concatenate([top, rest], 0), factor_x[lane, :, :GROUP], across,
                preferred_element_type=jnp.float32,
            )
            values = values[: STEP * WINDOW] + values[STEP * WINDOW :] + lax.dot_general(
                top, factor_x[lane, :, GROUP:], across, preferred_element_type=jnp.float32
            )
            for j in range(STEP):
                where = pl.ds(pl.multiple_of((first + j) * rows + start, 8), WINDOW)
                tile[where, :] += values[j * WINDOW : (j + 1) * WINDOW, :]

        return over_windows((low_z, high_z, low_y, high_y), group, visit)

    over_groups(atoms, prepare)


def interpolate_kernel(
    rows, grid, bits, count, low_z, high_z, low_y, high_y, key, charge, fz, fy, fx, tile, force_z, force_y, force_x,
    places, factor_x, table_z, rising_z, total,
):
    force_z[...] = jnp.zeros_like(force_z)
    force_y[...] = jnp.zeros_like(force_y)
    force_x[...] = jnp.zeros_like(force_x)
    fill_places(places)
    atoms = count[0]

    def prepare(group, lane):
        at = pl.ds(pl.multiple_of(group * GROUP, GROUP), GROUP)
        place = group * GROUP + lax.broadcasted_iota(jnp.int32, (1, GROUP), 1)
        value = -jnp.where(place < atoms, charge[0:1, at], 0.0)
        cell_z, cell_y, cell_x = decode(key[0:1, at], *bits)
        weight_z, slope_z = spline_weights(fz[0:1, at])
        weight_y, slope_y = spline_weights(fy[0:1, at])
        weight_x, slope_x = spline_weights(fx[0:1, at])
        for half, values in enumerate((weight_x, slope_x)):
            top, rest = wrapped_stencil(places[...], cell_x, values, grid)
            columns = slice(half * GROUP, (half + 1) * GROUP)
            factor_x[lane, :grid, columns] = top
            factor_x[lane, grid:, columns] = rest
        total[lane] = jnp.zeros(total.shape[1:], jnp.float32)

        def visit(first, start):
            span = table_z.shape[1]
            table_z[lane] = stencil(cell_z - first, weight_z, span)
            rising_z[lane] = stencil(cell_z - first, slope_z, span)
            top, rest = split(
                jnp.concatenate(
                    [
                        tile[pl.ds(pl.multiple_of((first + j) * rows + start, 8), WINDOW), :]
                        for j in range(STEP)
                    ],
                    0,
                )
            )
            along = jnp.dot(
                jnp.concatenate([top, rest], 0), factor_x[lane, :grid, :],
                preferred_element_type=jnp.float32,
            )
            along = along[: STEP * WINDOW] + along[STEP * WINDOW :] + jnp.dot(
                top, factor_x[lane, grid:, :], preferred_element_type=jnp.float32
            )
            table_y = stencil(cell_y - start, weight_y, WINDOW)
            rising_y = stencil(cell_y - start, slope_y, WINDOW)
            zs = [table_z[lane, j : j + 1, :] for j in range(STEP)]
            gs = [rising_z[lane, j : j + 1, :] for j in range(STEP)]
            sums = [0.0, 0.0, 0.0]
            for r in range(0, WINDOW, 8):
                local = slice(r, r + 8)
                w = [along[j * WINDOW + r : j * WINDOW + r + 8, :GROUP] for j in range(STEP)]
                s = [along[j * WINDOW + r : j * WINDOW + r + 8, GROUP:] for j in range(STEP)]
                sums[0] += table_y[local] * sum(gs[j] * w[j] for j in range(STEP))
                sums[1] += rising_y[local] * sum(zs[j] * w[j] for j in range(STEP))
                sums[2] += table_y[local] * sum(zs[j] * s[j] for j in range(STEP))
            for i in range(3):
                total[lane, 8 * i : 8 * i + 8, :] += sums[i]

        rest_of = over_windows((low_z, high_z, low_y, high_y), group, visit)

        def finish():
            rest_of()
            for i, force in enumerate((force_z, force_y, force_x)):
                part = total[lane, 8 * i : 8 * i + 8, :]
                force[0:1, at] = value * jnp.sum(part, 0, keepdims=True)

        return finish

    over_groups(atoms, prepare)


def vmem():
    return pl.BlockSpec(memory_space=pltpu.VMEM)


def smem():
    return pl.BlockSpec(memory_space=pltpu.SMEM)


def sort_rows_kernel(bits, count, fractions, cells, key, fz, fy, fx):
    slot = lax.broadcasted_iota(jnp.int32, key.shape, 1)
    packed = encode([cells[i : i + 1, :] for i in range(3)], *bits)
    key[...] = jnp.where(slot < count[0], packed, DEAD)
    for i, row in enumerate((fz, fy, fx)):
        row[...] = fractions[i : i + 1, :]


def sort_rows(count, fractions, cells, bits):
    slots = cells.shape[1]
    outs = pl.pallas_call(
        functools.partial(sort_rows_kernel, bits),
        out_shape=[jax.ShapeDtypeStruct((1, slots), jnp.int32)]
        + [jax.ShapeDtypeStruct((1, slots), jnp.float32)] * 3,
        in_specs=[smem()] + [vmem()] * 2,
        out_specs=[vmem()] * 4,
        cost_estimate=pl.CostEstimate(
            flops=20 * slots, bytes_accessed=40 * slots, transcendentals=0
        ),
        name="sort_rows",
    )(count, fractions, cells)
    return [row.reshape(slots) for row in outs]


def spread_atoms(count, bounds, atoms, bits, planes, rows, grid):
    slots = atoms[0].shape[1]
    return pl.pallas_call(
        functools.partial(spread_kernel, rows, grid, bits),
        out_shape=jax.ShapeDtypeStruct((planes * rows, grid), jnp.float32),
        in_specs=[smem()] * 5 + [vmem()] * 5,
        out_specs=vmem(),
        scratch_shapes=[
            pltpu.VMEM((grid, GROUP), jnp.bfloat16),
            pltpu.VMEM((PAIR, 8, GROUP), jnp.float32),
            pltpu.VMEM((PAIR, grid, 2 * GROUP), jnp.bfloat16),
        ],
        cost_estimate=pl.CostEstimate(
            flops=STEP * rows * grid * slots * 6,
            bytes_accessed=planes * rows * grid * 4,
            transcendentals=0,
        ),
        compiler_params=pltpu.CompilerParams(

        ),
        name="spread",
    )(count, *bounds, *atoms)


def interpolate_atoms(count, bounds, atoms, tile, bits, planes, rows, grid):
    slots = atoms[0].shape[1]
    return pl.pallas_call(
        functools.partial(interpolate_kernel, rows, grid, bits),
        out_shape=[jax.ShapeDtypeStruct((1, slots), jnp.float32)] * 3,
        in_specs=[smem()] * 5 + [vmem()] * 6,
        out_specs=[vmem()] * 3,
        scratch_shapes=[
            pltpu.VMEM((grid, GROUP), jnp.bfloat16),
            pltpu.VMEM((PAIR, 2 * grid, 2 * GROUP), jnp.bfloat16),
            pltpu.VMEM((PAIR, 8, GROUP), jnp.float32),
            pltpu.VMEM((PAIR, 8, GROUP), jnp.float32),
            pltpu.VMEM((PAIR, 24, GROUP), jnp.float32),
        ],
        cost_estimate=pl.CostEstimate(
            flops=STEP * rows * grid * slots * 12,
            bytes_accessed=planes * rows * grid * 4,
            transcendentals=0,
        ),
        name="interpolate",
    )(count, *bounds, *atoms, tile)


def turns(grid, wave, place, quarter):
    whole = np.mod(wave * place + (grid // 4) * quarter, grid)
    return np.cos(2.0 * np.pi * whole / grid).astype(np.float32)


def wave_tables(grid, slabs, columns, waves):
    kx = np.arange(slabs * waves).reshape(slabs, 1, waves)
    part = np.arange(2)
    x = np.arange(grid)
    table_x = turns(grid, kx[None], x[:, None, None, None], part[None, None, :, None])
    kz = np.arange(grid).reshape(columns, 1, grid // columns, 1, 1)
    table_z = turns(
        grid, kz, x[None, None, None, :, None],
        part[None, :, None, None, None] - part[None, None, None, None, :],
    ).reshape(2 * grid, 2 * grid)
    y = np.arange(grid).reshape(columns, 1, grid // columns, 1, 1)
    table_y = turns(
        grid, x[None, None, None, None, :], y,
        part[None, None, None, :, None] - part[None, :, None, None, None],
    )
    return table_x, table_z, table_y


def signed_wave(waves, grid):
    return jnp.where(waves < grid // 2, waves, waves - grid)


def influence(moduli, screening, slab, column, grid, count_kx, count_kz):
    kx = slab * count_kx + lax.iota(jnp.int32, count_kx)
    kz = column * count_kz + lax.iota(jnp.int32, count_kz)
    ky = lax.iota(jnp.int32, grid)
    half = grid // 2
    share = jnp.where((kx == 0) | (kx == half), 1.0, 2.0)
    share = jnp.where(kx <= half, share, 0.0) * (0.5 * coulomb / grid**3)
    nx, nz, ny = (signed_wave(k, grid) for k in (kx, kz, ky))
    radius = (nz * nz)[:, None, None] + (nx * nx)[None, :, None] + (ny * ny)[None, None, :]
    squared = radius.astype(jnp.float32) / float(grid * grid)
    mirrored = jnp.roll(moduli[:, ::-1], 1, 1)
    spare = jnp.zeros((count_kx * lax.axis_size("gz"),), jnp.float32)

    def product(table):
        mx = lax.dynamic_slice_in_dim(
            jnp.concatenate([table[2], spare]), slab * count_kx, count_kx, 0
        )
        mz = lax.dynamic_slice_in_dim(table[0], column * count_kz, count_kz, 0)
        return mz[:, None, None] * (share * mx)[None, :, None] * table[1][None, None, :]

    both = product(moduli) + product(mirrored)
    safe = jnp.where(radius > 0, squared, 1.0)
    return jnp.where(radius > 0, both * jnp.exp(-screening[0] * squared) / safe, 0.0)


def exchange(x, axis):
    return lax.all_to_all(x, axis, split_axis=0, concat_axis=0, tiled=True)


def contract(form, *operands):
    return jnp.einsum(form, *operands, precision=high, preferred_element_type=jnp.float32)


def potential_field(block, kernel, tables, slabs, columns, waves):
    table_x, table_z, table_y = tables
    planes, rows, grid = block.shape
    lanes = waves * rows
    spectrum = contract("zyx,xpck->pzcky", block, table_x)
    spectrum = exchange(spectrum.reshape(slabs * planes * 2, lanes), "gz")
    spectrum = contract("mn,nl->ml", table_z, spectrum)
    spectrum = exchange(spectrum, "gy").reshape(columns, 2, grid // columns, waves, rows)
    spectrum = contract("pczky,pcydw->zkdw", spectrum, table_y)
    spectrum = spectrum * kernel[:, :, None, :]
    spectrum = contract("zkdw,pcydw->pczky", spectrum, table_y)
    spectrum = exchange(spectrum.reshape(2 * grid, lanes), "gy")
    spectrum = contract("mn,ml->nl", table_z, spectrum)
    spectrum = exchange(spectrum, "gz").reshape(slabs, planes, 2, waves, rows)
    return contract("pzcky,xpck->zyx", spectrum, table_x)


LANES = 128
MESH = pl.DeviceIdType.MESH


def fast_sizes(slabs, columns, planes, rows, grid):
    return (
        2 * rows == LANES
        and grid == 2 * LANES
        and columns * rows == grid
        and slabs * planes == grid
        and planes % 8 == 0
        and LANES % (2 * columns) == 0
        and LANES % slabs == 0
        and slabs >= 3
        and columns >= 3
    )


def kept_waves(half, columns):
    pairs = [k for n in range(1, half // 2) for k in (n, half - n)]
    return np.array([0, half // 2] + pairs).reshape(columns, half // columns)


def partners(half, columns):
    share = half // columns
    moves = np.zeros((columns, 2 * share, 2 * share), np.float32)
    for c, waves in enumerate(kept_waves(half, columns)):
        place = {int(k): j for j, k in enumerate(waves)}
        for h in range(2):
            for k, j in place.items():
                other = (2 * half - h * half - k) % (2 * half)
                moves[c, h * share + j, other // half * share + place[other % half]] = 1.0
    return moves.astype(jnp.bfloat16)


def fill_green(green, moduli, screening, slab, column, waves, columns):
    grid = moduli.shape[1]
    half = grid // 2
    share = half // columns
    tall = 2 * share

    def signed(k):
        return jnp.where(k < half, k, k - grid)

    def opposite(k):
        return jnp.where(k == 0, 0, grid - k)

    def pick(lanes, at, values):
        return jnp.sum(jnp.where(lanes == at, values, 0.0), 1, keepdims=True)

    down = lax.broadcasted_iota(jnp.int32, (grid, grid), 0)
    over = lax.broadcasted_iota(jnp.int32, (grid, grid), 1)
    turned = pick(over, opposite(down), moduli[1:2, :])
    factor_y = moduli[1:2, :]
    mirror_y = jnp.sum(jnp.where(down == over, turned, 0.0), 0, keepdims=True)
    lanes = over[:tall]
    row = down[:tall]
    upper = jnp.where(row >= share, 1, 0)
    place = column * share + row - upper * share
    kept = jnp.where((place & 1) == 0, place >> 1, half - (place >> 1))
    kz = upper * half + jnp.where(place == 1, half // 2, kept)
    factor_z = pick(lanes, kz, moduli[0:1, :])
    mirror_z = pick(lanes, opposite(kz), moduli[0:1, :])
    flat = signed(kz) * signed(kz) + signed(lanes) * signed(lanes)

    def values(kx):
        share_x = jnp.where((kx == 0) | (kx == half), 1.0, 2.0) * (0.5 * coulomb / grid**3)
        factor_x = share_x * pick(over[:1], kx, moduli[2:3, :])
        mirror_x = share_x * pick(over[:1], opposite(kx), moduli[2:3, :])
        both = factor_x * factor_z * factor_y + mirror_x * mirror_z * mirror_y
        radius = flat + signed(kx) * signed(kx)
        squared = radius.astype(jnp.float32) * (1.0 / (grid * grid))
        safe = jnp.where(radius > 0, squared, 1.0)
        return jnp.where(radius > 0, both * jnp.exp(-screening[0] * squared) / safe, 0.0)

    plain = values(slab * waves)
    ends = values(half)
    green[:tall, :] = jnp.where(slab == 0, 0.5 * (plain + ends), plain)
    green[waves * tall :, :] = jnp.where(slab == 0, 0.5 * (plain - ends), 0.0)

    @pl.loop(1, waves)
    def _(w):
        green[pl.ds(pl.multiple_of(w * tall, tall), tall), :] = values(slab * waves + w)


def halves(table):
    table = np.ascontiguousarray(table, dtype=np.float32)
    top = table.astype(jnp.bfloat16)
    rest = (table - top.astype(np.float32)).astype(jnp.bfloat16)
    return top, rest


def solve_tables(grid, slabs, columns, waves, planes):
    half = grid // 2
    pairs = planes // 2
    share = half // columns
    x = np.arange(grid)
    part = np.arange(2)
    kx = np.repeat(np.arange(slabs * waves), 2)
    px = np.tile(part, slabs * waves)
    table_x = turns(grid, kx[:, None], x[None, :], px[:, None])
    table_x[1] = np.where(x % 2, -1.0, 1.0)
    forward_x = np.concatenate(halves(table_x))
    inverse_x = np.concatenate(halves(table_x.T))
    kept = kept_waves(half, columns)
    kz = np.broadcast_to(kept[:, None, :], (columns, 2, share)).reshape(-1)
    pk = np.broadcast_to(part.reshape(1, 2, 1), (columns, 2, share)).reshape(-1)
    zh = np.broadcast_to(np.arange(half).reshape(slabs, 1, pairs), (slabs, 2, pairs)).reshape(-1)
    pz = np.broadcast_to(part.reshape(1, 2, 1), (slabs, 2, pairs)).reshape(-1)
    table_z = turns(half, kz[:, None], zh[None, :], pk[:, None] - pz[None, :])
    forward_z = np.stack(halves(table_z))
    inverse_z = np.stack(halves(table_z.T))
    ky = np.tile(np.arange(grid), 2)
    pf = np.repeat(part, grid)
    table_y = turns(grid, ky[:, None], ky[None, :], pf[None, :] - pf[:, None])
    forward_y = np.stack(halves(table_y))
    angle = 2.0 * np.pi * kept.reshape(-1, 1) / grid
    upper = np.arange(LANES)[None, :] >= LANES // 2
    twist = np.stack(
        [np.where(upper, np.cos(angle), 1.0), np.where(upper, np.sin(angle), 0.0)]
    ).astype(np.float32)
    return forward_x, inverse_x, forward_z, inverse_z, forward_y, twist, partners(half, columns)


def chunks_of(waves, count):
    edges = [waves * i // count for i in range(count + 1)]
    return [(a, b - a) for a, b in zip(edges, edges[1:]) if b > a]


def solve_kernel(
    slabs, columns, waves, planes, rows, grid, chunks,
    tile, moduli, screening, table_fx, *rest_of,
):
    late, out, green = rest_of[:6], rest_of[6], rest_of[7]
    tables, table_sems = rest_of[8:14], rest_of[14]
    (
        rim_z, rim_y, rim_c,
        x_out, z_in, z_out, y_in, y_out, z_back, z_send, x_in, y_top, y_rest, y_right,
        rim_send, rim_recv, gz_send, gz_recv, gy_send, gy_recv, by_send, by_recv, bz_send, bz_recv,
    ) = rest_of[15:]
    table_ix, table_fz, table_iz, table_y, twist, moves = tables
    half = grid // 2
    pairs = planes // 2
    wide = 2 * pairs
    share = half // columns
    tall = 2 * share
    bins = 2 * slabs * waves
    slab = lax.axis_index("gz")
    column = lax.axis_index("gy")

    def around(step):
        return lax.rem(slab + step + slabs, slabs)

    def beside(step):
        return lax.rem(column + step + columns, columns)

    barrier = pltpu.get_barrier_semaphore()
    for step in range(1, slabs):
        pl.semaphore_signal(barrier, inc=1, device_id=(around(step), column), device_id_type=MESH)
    for step in range(1, columns):
        pl.semaphore_signal(barrier, inc=1, device_id=(slab, beside(step)), device_id_type=MESH)
    for step in (1, -1):
        pl.semaphore_signal(
            barrier, inc=1, device_id=(around(step), beside(step)), device_id_type=MESH
        )
    pl.semaphore_wait(barrier, slabs + columns)

    def remote(source, target, sends, recvs, at, to):
        return pltpu.make_async_remote_copy(
            src_ref=source, dst_ref=target, send_sem=sends.at[at], recv_sem=recvs.at[at],
            device_id=to, device_id_type=MESH,
        )

    main, edge = pl.ds(0, rows), pl.ds(rows, 8)
    body_z, over_z = pl.ds(0, planes), pl.ds(planes, 3)
    rims = [
        remote(tile.at[over_z, main], rim_z, rim_send, rim_recv, 0, (around(1), column)),
        remote(tile.at[body_z, edge], rim_y, rim_send, rim_recv, 1, (slab, beside(1))),
        remote(tile.at[over_z, edge], rim_c, rim_send, rim_recv, 2, (around(1), beside(1))),
    ]
    for copy in rims:
        copy.start()
    fetches = [
        pltpu.make_async_copy(source, target, table_sems.at[i])
        for i, (source, target) in enumerate(zip(late, tables))
    ]
    for fetch in fetches:
        fetch.start()

    out[planes + 3 :] = jnp.zeros_like(out[planes + 3 :])
    across = (((1,), (1,)), ((), ()))

    def product(left, right, form=(((1,), (0,)), ((), ()))):
        return lax.dot_general(left, right, form, preferred_element_type=jnp.float32)

    def along_x(at, rim):
        value = tile[pl.ds(at * 4, 4), :rows, :]
        head = value[:, :8] + rim_y[pl.ds(at * 4, 4)]
        value = jnp.concatenate([head, value[:, 8:]], 1)
        if rim is not None:
            value = value + jnp.concatenate([rim, jnp.zeros((1, rows, grid), jnp.float32)], 0)
        top, rest = split(value.reshape(4 * rows, grid))
        both = product(table_fx[...], top, across)
        values = both[:bins] + both[bins:] + product(table_fx[:bins, :], rest, across)
        for side in range(2):
            where = pl.ds(2 * at + side, bins, stride=pairs)
            x_out[where, :] = values[:, side * LANES : (side + 1) * LANES]

    rims[1].wait()

    @pl.loop(0, (planes // 4 - 2) // 2)
    def _(turn_at):
        along_x(2 * turn_at + 1, None)
        along_x(2 * turn_at + 2, None)

    rims[0].wait()
    rims[2].wait()
    rim_z[:, :8, :] += rim_c[...]
    along_x(planes // 4 - 1, None)
    along_x(0, rim_z[...])

    def gz_copy(q, step):
        w, n = chunks[q]
        source = x_out.at[pl.ds((around(step) * waves + w) * wide, n * wide)]
        target = z_in.at[slab, pl.ds(w * wide, n * wide)]
        return remote(source, target, gz_send, gz_recv, (q, step), (around(step), column))

    def gy_copy(q, step):
        w, n = chunks[q]
        where = pl.ds(w * tall, n * tall)
        source, target = z_out.at[beside(step), where], y_in.at[column, where]
        return remote(source, target, gy_send, gy_recv, (q, step), (slab, beside(step)))

    def by_copy(q, step):
        w, n = chunks[q]
        where = pl.ds(w * tall, n * tall)
        source, target = y_out.at[beside(step), where], z_back.at[column, where]
        return remote(source, target, by_send, by_recv, (q, step), (slab, beside(step)))

    def bz_copy(q, step):
        w, n = chunks[q]
        source = z_send.at[around(step), pl.ds(w * wide, n * wide)]
        target = x_in.at[pl.ds((slab * waves + w) * wide, n * wide)]
        return remote(source, target, bz_send, bz_recv, (q, step), (around(step), column))

    for q in range(len(chunks)):
        for step in range(1, slabs):
            gz_copy(q, step).start()
    z_in[slab] = x_out[pl.ds(pl.multiple_of(slab * waves * wide, wide), waves * wide), :]

    for fetch in fetches:
        fetch.wait()
    fill_green(green, moduli, screening, slab, column, waves, columns)
    left = lax.broadcasted_iota(jnp.int32, (half, LANES), 1) < LANES // 2
    side = left[:share]

    def turn(value):
        return pltpu.roll(value, LANES // 2, 1)

    def along_z(table, value):
        top, rest = split(value)
        both = product(table[0], jnp.concatenate([top, rest], 1))
        return both[:, :LANES] + both[:, LANES:] + product(table[1], top)

    def to_z(q):
        for step in range(1, slabs):
            gz_copy(q, step).wait_recv()
        first, count = chunks[q]

        @pl.loop(first, first + count)
        def _(w):
            value = z_in[:, pl.ds(pl.multiple_of(w * wide, wide), wide), :].reshape(grid, LANES)
            value = along_z(table_fz, value)
            value = value.reshape(columns, 2, share, LANES)
            re = value[:, 0].reshape(half, LANES)
            im = value[:, 1].reshape(half, LANES)
            re, im = re * twist[0] + im * twist[1], im * twist[0] - re * twist[1]
            for p, v in enumerate((re, im)):
                v = jnp.where(left, v + turn(v), turn(v) - v)
                where = pl.ds(pl.multiple_of(w * tall + p * share, share), share)
                z_out[:, where, :] = v.reshape(columns, share, LANES)

        for step in range(1, columns):
            gy_copy(q, step).start()
        where = pl.ds(first * tall, count * tall)
        y_in[column, where, :] = z_out[column, where, :]

    def to_y(q):
        for step in range(1, columns):
            gy_copy(q, step).wait_recv()
        first, count = chunks[q]

        @pl.loop(0, count)
        def _(w):
            for p in range(2):
                where = pl.ds(pl.multiple_of((first + w) * tall + p * share, share), share)
                for c in range(0, columns, 2):
                    a, b = y_in[c, where, :], y_in[c + 1, where, :]
                    pair = (jnp.where(side, a, turn(b)), jnp.where(side, turn(a), b))
                    for h in range(2):
                        to = pl.ds(pl.multiple_of(w * tall + h * share, share), share)
                        at = (p * columns + c) * rows
                        top, rest = split(pair[h])
                        y_top[to, at : at + LANES] = top
                        y_rest[to, at : at + LANES] = rest

        main_rows = size = count * tall
        if first == 0:
            size += tall
            for target in (y_top, y_rest):
                value = product(moves[column], target[:tall, :])
                value = jnp.concatenate([value[:, :grid], -value[:, grid:]], 1)
                target[main_rows:size, :] = value.astype(jnp.bfloat16)
        top = y_top[:size, :]
        both = product(jnp.concatenate([top, y_rest[:size, :]], 0), table_y[0])
        value = both[:size] + both[size:] + product(top, table_y[1])
        factor = green[first * tall : (first + count) * tall, :]
        if first == 0:
            factor = jnp.concatenate([factor, green[waves * tall :, :]], 0)
        value = jnp.concatenate([value[:, :grid] * factor, value[:, grid:] * factor], 1)
        if first == 0:
            value = jnp.concatenate([value[:tall] + value[main_rows:], value[tall:main_rows]], 0)
        size = main_rows
        top, rest = split(value)
        both = product(jnp.concatenate([top, rest], 0), table_y[0], across)
        y_right[:size, :] = both[:size] + both[size:] + product(top, table_y[1], across)

        @pl.loop(0, count)
        def _(w):
            for p in range(2):
                where = pl.ds(pl.multiple_of((first + w) * tall + p * share, share), share)
                for c in range(0, columns, 2):
                    at = (p * columns + c) * rows
                    a, b = (
                        y_right[
                            pl.ds(pl.multiple_of(w * tall + h * share, share), share),
                            at : at + LANES,
                        ]
                        for h in range(2)
                    )
                    y_out[c, where, :] = jnp.where(side, a, turn(b))
                    y_out[c + 1, where, :] = jnp.where(side, turn(a), b)

        for step in range(1, columns):
            by_copy(q, step).start()
        where = pl.ds(first * tall, count * tall)
        z_back[column, where, :] = y_out[column, where, :]

    def from_z(q):
        for step in range(1, columns):
            by_copy(q, step).wait_recv()
        first, count = chunks[q]

        @pl.loop(first, first + count)
        def _(w):
            value = z_back[:, pl.ds(pl.multiple_of(w * tall, tall), tall), :]
            re = value[:, :share].reshape(half, LANES)
            im = value[:, share:].reshape(half, LANES)
            re, im = (jnp.where(left, v + turn(v), turn(v) - v) for v in (re, im))
            re, im = re * twist[0] - im * twist[1], im * twist[0] + re * twist[1]
            re, im = (v.reshape(columns, share, LANES) for v in (re, im))
            value = jnp.concatenate(
                [v[c] for c in range(columns) for v in (re, im)], 0
            )
            value = along_z(table_iz, value)
            where = pl.ds(pl.multiple_of(w * wide, wide), wide)
            z_send[:, where, :] = value.reshape(slabs, wide, LANES)

        for step in range(1, slabs):
            bz_copy(q, step).start()
        where = pl.ds(pl.multiple_of((slab * waves + first) * wide, wide), count * wide)
        x_in[where, :] = z_send[slab, pl.ds(first * wide, count * wide), :]

    stages = (to_z, to_y, from_z)
    for turn_at in range(len(chunks) + len(stages) - 1):
        for at, stage in enumerate(stages):
            if 0 <= turn_at - at < len(chunks):
                stage(turn_at - at)
    for q in range(len(chunks)):
        for step in range(1, slabs):
            bz_copy(q, step).wait_recv()

    def back_x(at):
        value = jnp.concatenate(
            [x_in[pl.ds(2 * at + s, bins, stride=pairs), :] for s in range(2)], 1
        )
        top, rest = split(value)
        both = product(table_ix[...], top)
        value = both[:grid] + both[grid:] + product(table_ix[:grid, :], rest)
        out[pl.ds(at * 4, 4), :rows, :] = value.T.reshape(4, rows, grid)

    def rim_back(at):
        planes_of = pl.ds(8 * at, 8)
        return remote(
            out.at[planes_of, pl.ds(0, 8)], out.at[planes_of, edge],
            rim_send, rim_recv, 5 + at, (slab, beside(-1)),
        )

    rims_back = [rim_back(at) for at in range(planes // 8)] + [
        remote(
            out.at[pl.ds(0, 3), main], out.at[over_z, main],
            rim_send, rim_recv, 3, (around(-1), column),
        ),
        remote(
            out.at[pl.ds(0, 3), pl.ds(0, 8)], out.at[over_z, edge],
            rim_send, rim_recv, 4, (around(-1), beside(-1)),
        ),
    ]
    for at in range(planes // 8):
        back_x(2 * at)
        back_x(2 * at + 1)
        if at == 0:
            for copy in rims_back[-2:]:
                copy.start()
        else:
            rims_back[at - 1].start()
    rims_back[planes // 8 - 1].start()
    for q in range(len(chunks)):
        for copy, steps in (
            (gz_copy, slabs), (gy_copy, columns), (by_copy, columns), (bz_copy, slabs)
        ):
            for step in range(1, steps):
                copy(q, step).wait_send()
    for copy in rims_back:
        copy.wait()


def solve_fused(tile, moduli, screening, slabs, columns, planes, rows, waves):
    span_planes, span_rows, grid = tile.shape
    tables = solve_tables(grid, slabs, columns, waves, planes)
    chunks = chunks_of(waves, CHUNKS)
    most = max(n for _, n in chunks)
    wide, tall = planes, 2 * (grid // 2 // columns)

    def scratch(*shape):
        return pltpu.VMEM(shape, jnp.float32)

    def narrow(*shape):
        return pltpu.VMEM(shape, jnp.bfloat16)

    def flags(count):
        return [pltpu.SemaphoreType.DMA((len(chunks), count))] * 2

    return pl.pallas_call(
        functools.partial(
            solve_kernel, slabs, columns, waves, planes, rows, grid, chunks
        ),
        out_shape=jax.ShapeDtypeStruct(tile.shape, jnp.float32),
        in_specs=[vmem()] * 2 + [smem(), vmem()]
        + [pl.BlockSpec(memory_space=pl.ANY)] * 6,
        out_specs=vmem(),
        scratch_shapes=[
            scratch((waves + 1) * tall, grid),
            *[pltpu.VMEM(t.shape, t.dtype) for t in tables[1:]],
            pltpu.SemaphoreType.DMA((6,)),
            scratch(3, rows, grid), scratch(planes, 8, grid), scratch(3, 8, grid),
            scratch(slabs * waves * wide, LANES), scratch(slabs, waves * wide, LANES),
            scratch(columns, waves * tall, LANES), scratch(columns, waves * tall, LANES),
            scratch(columns, waves * tall, LANES), scratch(columns, waves * tall, LANES),
            scratch(slabs, waves * wide, LANES), scratch(slabs * waves * wide, LANES),
            narrow((most + 1) * tall, 2 * grid), narrow((most + 1) * tall, 2 * grid),
            scratch(most * tall, 2 * grid),
            *[pltpu.SemaphoreType.DMA((5 + planes // 8,))] * 2,
            *flags(slabs), *flags(columns), *flags(columns), *flags(slabs),
        ],
        compiler_params=pltpu.CompilerParams(
            collective_id=0, has_side_effects=True, vmem_limit_bytes=60 * 1024 * 1024
        ),
        cost_estimate=pl.CostEstimate(
            flops=10**10, bytes_accessed=span_planes * span_rows * grid * 8, transcendentals=0
        ),
        name="solve",
    )(tile, moduli, screening, *(jnp.asarray(t) for t in tables))


def solve_tile(volume, kernel, tables, planes, rows, waves, slabs, columns):
    span_planes, span_rows, grid = volume.shape
    rim_planes = shifted(volume[planes : planes + 3], "gz", 1)
    volume = jnp.concatenate([volume[:3] + rim_planes, volume[3:planes]], 0)
    rim_rows = shifted(volume[:, rows : rows + 3], "gy", 1)
    block = jnp.concatenate([volume[:, :3] + rim_rows, volume[:, 3:rows]], 1)
    potential = potential_field(block, kernel, tables, slabs, columns, waves)
    upper_rows = shifted(potential[:, :3], "gy", -1)
    spare_rows = jnp.zeros((planes, span_rows - rows - 3, grid), jnp.float32)
    widened = jnp.concatenate([potential, upper_rows, spare_rows], 1)
    upper_planes = shifted(widened[:3], "gz", -1)
    spare_planes = jnp.zeros((span_planes - planes - 3, span_rows, grid), jnp.float32)
    return jnp.concatenate([widened, upper_planes, spare_planes], 0)


def body(charge, fractions, cell_base, live_blocks, send_blocks, moduli, screening):
    slabs = lax.axis_size("gz")
    columns = lax.axis_size("gy")
    grid = moduli.shape[1]
    planes = grid // slabs
    rows = grid // columns
    span_planes = round_up(planes + 3 + STEP, 2)
    span_rows = round_up(rows + 3, 8)
    waves = -(-(grid // 2 + 1) // slabs)
    slab = lax.axis_index("gz")
    column = lax.axis_index("gy")
    lane_ids = lax.iota(jnp.int32, columns)
    live = jnp.sum(jnp.where(lane_ids == column, live_blocks[0], 0))
    send = jnp.sum(jnp.where(lane_ids == column, send_blocks[0], 0))
    kept_atoms = (live - send) * BLOCK
    live_atoms = live * BLOCK
    slots = charge.shape[0]
    bits = ((rows - 1).bit_length(), (grid - 1).bit_length())
    slot = lax.iota(jnp.int32, slots)
    count = live_atoms[None]
    key, *steps = sort_rows(count, fractions, cell_base, bits)
    key, slot, *values = lax.sort((key, slot, charge, *steps), num_keys=1, is_stable=False)
    by_group = key.reshape(slots // GROUP, GROUP)
    alive = by_group < DEAD
    cell_z, cell_y, _ = decode(by_group, *bits)
    bounds = []
    for cell in (cell_z, cell_y):
        high = jnp.max(jnp.where(alive, cell, 0), 1)
        bounds += [jnp.min(jnp.where(alive, cell, high[:, None]), 1), high]
    atoms = [v[None, :] for v in (key, *values)]
    sizes = (span_planes, span_rows, grid)
    tile = spread_atoms(count, bounds, atoms, bits, *sizes).reshape(sizes)
    if fast_sizes(slabs, columns, planes, rows, grid):
        packed_waves = grid // 2 // slabs
        padded = solve_fused(tile, moduli, screening, slabs, columns, planes, rows, packed_waves)
    else:
        tables = wave_tables(grid, slabs, columns, waves)
        kernel = influence(moduli, screening, slab, column, grid, waves, grid // columns)
        padded = solve_tile(tile, kernel, tables, planes, rows, waves, slabs, columns)
    padded = padded.reshape(span_planes * span_rows, grid)
    forces = interpolate_atoms(count, bounds, atoms, padded, bits, *sizes)
    _, *home = lax.sort((slot, *(f[0] for f in forces)), num_keys=1, is_stable=False)
    home = jnp.stack(home)
    margin = SEND_MAX * BLOCK
    room = jnp.concatenate([home, jnp.zeros((3, margin), jnp.float32)], 1)
    lent = lax.dynamic_slice_in_dim(room, kept_atoms, margin, 1)
    moved = shifted(lent, "gy", 1)
    kept = jnp.where(lax.iota(jnp.int32, slots) < kept_atoms, home, 0.0)
    holder = jnp.zeros((3, slots + margin), jnp.float32)
    holder = lax.dynamic_update_slice(holder, moved, (jnp.zeros((), jnp.int32), kept_atoms))
    return kept + holder[:, :slots]


def solution(mesh):
    return jax.shard_map(
        body,
        mesh=mesh,
        in_specs=(
            P(("gz", "gy")),
            P(None, ("gz", "gy")),
            P(None, ("gz", "gy")),
            P("gz", None),
            P("gz", None),
            P(),
            P(),
        ),
        out_specs=P(None, ("gz", "gy")),
        check_vma=False,
    )
```
